128 devices in a mesh: frame: 8 (over x, core), seq: 16 (over y, z).
Axes of the slice: x: 4, y: 4, z: 4, core: 2. Of those that a mesh axis runs over, the one named last changes fastest.
Arguments:
- vit_states: bfloat16 [256, 256, 1280], P(('frame', 'seq')), may hold values from -6 to 6
- frame_slot: int32 [128], replicated, may hold values from 0 to 255, as said below
- patch_count: int32 [128], replicated, may hold values from 208 to 256, as said below
- vis_start: int32 [128], replicated, may hold values from 0 to 16383, as said below
- text_embed: bfloat16 [128, 128, 4096], P(None, ('frame', 'seq')), may hold values from -6 to 6
- vit_ln_gain: float32 [1280], replicated, may hold values from 0.25 to 1.75
- vit_ln_bias: float32 [1280], replicated, may hold values from -1.5 to 1.5
- vit_qkv_w: bfloat16 [1280, 3840], P('seq'), may hold values from -0.15625 to 0.15625
- vit_qkv_b: float32 [3840], replicated, may hold values from -1.5 to 1.5
- vit_out_w: bfloat16 [1280, 1280], P('seq'), may hold values from -0.15625 to 0.15625
- vit_out_b: float32 [1280], replicated, may hold values from -1.5 to 1.5
- proj_w: bfloat16 [1280, 4096], replicated, may hold values from -0.15625 to 0.15625
- proj_b: float32 [4096], replicated, may hold values from -1.5 to 1.5
- attn_gain: float32 [4096], replicated, may hold values from 0.25 to 1.75
- wq: bfloat16 [4096, 2048], P(None, 'frame'), may hold values from -0.09375 to 0.09375
- wk: bfloat16 [4096, 1024], P(None, 'frame'), may hold values from -0.09375 to 0.09375
- wv: bfloat16 [4096, 1024], P(None, 'frame'), may hold values from -0.09375 to 0.09375
- wo: bfloat16 [2048, 4096], P('frame'), may hold values from -0.125 to 0.125
Outputs:
- mixed: bfloat16 [128, 128, 4096], P(None, ('frame', 'seq'))
The draws below stay inside these ranges and needn't reach their ends.
Inputs may be any that keep to these rules, and one draw needn't show every extreme that they name: Frame t sits in slot frame_slot[t]; slot k of the device with index d (axes frame then seq) is d * 2 + k; no slot holds two frames. The two devices with frame indices 2i and 2i+1 and the same seq index hold exactly two frames between them; some device holds 2 frames. `patch_count`: A multiple of 4; some frame has 256 patches. Frame t's patch_count[t] / 4 visual positions start at vis_start[t] and lie within positions t * 128 to (t + 1) * 128 - 1.
All inputs are finite; a program needn't handle non-finite values.
Results may differ from the reference program's by a relative error of at most 0.015.
Values may be sent and summed in bfloat16 or wider, within the bound.
A program may use at most 128 MiB of HBM per device.

```python
import math
import jax
import jax.numpy as jnp
from jax import lax

VW = 1280
VHEADS = 16
MODEL_WIDTH = 4096
QUERY_HEADS_HALF = 16
KEY_VALUE_HEADS = 8
HEAD_WIDTH = 128
FRAME_MAX = 256
SLOTS = 2
TOK_OWN = 128
VIS_MAX = 64
N_FRAME = 8
N_SEQ = 16
DEVICES = 128


def frame_spans(key):
    inner_key = jax.random.fold_in(key, 5)
    count_key, place_key = jax.random.split(inner_key)
    lowest = VIS_MAX - VIS_MAX // 5
    tokens = jax.random.randint(count_key, (DEVICES,), lowest, VIS_MAX + 1).astype(jnp.int32)
    tokens = tokens.at[0].set(VIS_MAX)
    spare = TOK_OWN - tokens
    offsets = jax.random.randint(place_key, (DEVICES,), 0, spare + 1).astype(jnp.int32)
    starts = jnp.arange(DEVICES).astype(jnp.int32) * TOK_OWN + offsets
    return (tokens * 4, starts)


def draw_patch_count(key, part):
    counts, starts = frame_spans(key)
    return counts


def draw_vis_start(key, part):
    counts, starts = frame_spans(key)
    return starts


def draw_frame_slot(key, part):
    pairs_n = DEVICES // 2
    order_key, slot_key = jax.random.split(jax.random.fold_in(key, 3))
    frames_perm = jax.random.permutation(order_key, DEVICES).astype(jnp.int32)
    scores = jax.random.randint(slot_key, (pairs_n, 4), 0, 1 << 20) * 4 + jnp.arange(4).astype(jnp.int32)[None, :]
    chosen = jnp.argsort(scores, axis=1)[:, :2].astype(jnp.int32)
    chosen = chosen.at[0].set(jnp.array([0, 1], jnp.int32))
    earlier_slot = jnp.min(chosen, axis=1)
    later_slot = jnp.max(chosen, axis=1)
    pair_ids = jnp.arange(pairs_n).astype(jnp.int32)
    low_device = pair_ids // N_SEQ * 2 * N_SEQ + pair_ids % N_SEQ
    first_slots = (low_device + earlier_slot // 2 * N_SEQ) * 2 + earlier_slot % 2
    second_slots = (low_device + later_slot // 2 * N_SEQ) * 2 + later_slot % 2
    result = jnp.zeros((DEVICES,), jnp.int32)
    result = result.at[frames_perm[0::2]].set(first_slots)
    result = result.at[frames_perm[1::2]].set(second_slots)
    return result


def level_of(own_key, dims, shards, smallest, largest):
    def one(position, shards_of):
        steps = jax.random.uniform(jax.random.fold_in(jax.random.fold_in(own_key, 6), position), (shards_of,), jnp.float32, smallest / len(shards), largest / len(shards))
        return jnp.repeat(jnp.exp(steps), dims[position] // shards_of).reshape((-1,) + (1,) * (len(dims) - position - 1))

    gain = one(*shards[0])
    for cut in shards[1:]:
        gain = gain * one(*cut)
    return gain


def normal_values(stream_key, extent, scale, limit, cuts=(), held_as=jnp.bfloat16):
    values = jax.random.normal(stream_key, extent, jnp.float32) * scale
    if len(cuts) > 0:
        values = level_of(stream_key, extent, cuts, -0.22, 0.18) * values
    return jnp.clip(values, min=-limit, max=limit).astype(held_as)


def setup_inputs(seed: int = 0) -> dict:
    key_list = jax.random.split(jax.random.key(seed), 19)
    return {
        "vit_states": normal_values(key_list[0], (DEVICES * SLOTS, FRAME_MAX, VW), 1.0, 6.0, ((0, 128),)),
        "frame_slot": draw_frame_slot(jax.random.fold_in(key_list[18], 71), 0),
        "patch_count": draw_patch_count(jax.random.fold_in(key_list[18], 71), 0),
        "vis_start": draw_vis_start(jax.random.fold_in(key_list[18], 71), 0),
        "text_embed": normal_values(key_list[4], (TOK_OWN, DEVICES, MODEL_WIDTH), 1.0, 6.0, ((1, 128),)),
        "vit_ln_gain": jnp.clip(1.0 + 0.15 * jax.random.normal(key_list[5], (VW,), jnp.float32), 0.25, 1.75),
        "vit_ln_bias": normal_values(key_list[6], (VW,), 0.3, 1.5, (), jnp.float32),
        "vit_qkv_w": normal_values(key_list[7], (VW, 3 * VW), VW ** -0.5, 0.15625, ((0, 16),)),
        "vit_qkv_b": normal_values(key_list[8], (3 * VW,), 0.3, 1.5, (), jnp.float32),
        "vit_out_w": normal_values(key_list[9], (VW, VW), VW ** -0.5, 0.15625, ((0, 16),)),
        "vit_out_b": normal_values(key_list[10], (VW,), 0.3, 1.5, (), jnp.float32),
        "proj_w": normal_values(key_list[11], (VW, MODEL_WIDTH), VW ** -0.5, 0.15625),
        "proj_b": normal_values(key_list[12], (MODEL_WIDTH,), 0.3, 1.5, (), jnp.float32),
        "attn_gain": jnp.clip(1.0 + 0.15 * jax.random.normal(key_list[13], (MODEL_WIDTH,), jnp.float32), 0.25, 1.75),
        "wq": normal_values(key_list[14], (MODEL_WIDTH, QUERY_HEADS_HALF * HEAD_WIDTH), MODEL_WIDTH ** -0.5, 0.09375, ((1, 8),)),
        "wk": normal_values(key_list[15], (MODEL_WIDTH, KEY_VALUE_HEADS * HEAD_WIDTH), MODEL_WIDTH ** -0.5, 0.09375, ((1, 8),)),
        "wv": normal_values(key_list[16], (MODEL_WIDTH, KEY_VALUE_HEADS * HEAD_WIDTH), MODEL_WIDTH ** -0.5, 0.09375, ((1, 8),)),
        "wo": normal_values(key_list[17], (QUERY_HEADS_HALF * HEAD_WIDTH, MODEL_WIDTH), (QUERY_HEADS_HALF * HEAD_WIDTH) ** -0.5, 0.125, ((0, 8),)),
    }


rope_theta = 500000.0
vit_epsilon = 1e-06
norm_epsilon = 1e-05
masked_score = -1e+30

def apply_rotary(values, rotary_angles):
    half_width = values.shape[-1] // 2
    first_half = values[..., :half_width]
    second_half = values[..., half_width:]
    cosine = jnp.cos(rotary_angles)
    sine_part = jnp.sin(rotary_angles)
    return jnp.concatenate([first_half * cosine - second_half * sine_part, second_half * cosine + first_half * sine_part], axis=-1)

def rope_angles(positions, head_size):
    exponents = jnp.arange(0, head_size, 2).astype(jnp.float32) / head_size
    inverse = jnp.power(jnp.float32(rope_theta), -exponents)
    return positions.astype(jnp.float32)[:, None] * inverse[None, :]

def vit_frame(states, patches, ln_gain, ln_bias, qkv_weight, qkv_bias, out_weight, out_bias):
    frame_max = states.shape[0]
    width_vit = states.shape[1]
    states_wide = states.astype(jnp.float32)
    average = lax.optimization_barrier(jnp.mean(states_wide, axis=1, keepdims=True))
    centred = states_wide - average
    spread = lax.optimization_barrier(jnp.mean(centred * centred, axis=1, keepdims=True))
    normed_states = (centred * lax.rsqrt(spread + vit_epsilon) * ln_gain + ln_bias).astype(jnp.bfloat16)
    projected = (jnp.dot(normed_states, qkv_weight, preferred_element_type=jnp.float32) + qkv_bias).astype(jnp.bfloat16)
    head_size = width_vit // VHEADS
    shaped = projected.reshape(frame_max, 3, VHEADS, head_size).astype(jnp.float32)
    scores = jnp.einsum('qhd,khd->hqk', shaped[:, 0], shaped[:, 1]) / math.sqrt(head_size)
    key_live = jnp.arange(frame_max).astype(jnp.int32) < patches
    scores = jnp.where(key_live[None, None, :], scores, masked_score)
    highest = lax.optimization_barrier(jnp.max(scores, axis=-1, keepdims=True))
    weights = jnp.exp(scores - highest)
    probabilities = (weights / lax.optimization_barrier(jnp.sum(weights, axis=-1, keepdims=True))).astype(jnp.bfloat16)
    context = jnp.einsum('hqk,khd->qhd', probabilities.astype(jnp.float32), shaped[:, 2]).astype(jnp.bfloat16)
    attended = jnp.dot(context.reshape(frame_max, width_vit), out_weight, preferred_element_type=jnp.float32)
    hidden = (states_wide + attended + out_bias).astype(jnp.bfloat16)
    return lax.optimization_barrier(jnp.mean(hidden.astype(jnp.float32).reshape(frame_max // 4, 4, width_vit), axis=1)).astype(jnp.bfloat16)

def reference(vit_states, frame_slot, patch_count, vis_start, text_embed, vit_ln_gain, vit_ln_bias, vit_qkv_w, vit_qkv_b, vit_out_w, vit_out_b, proj_w, proj_b, attn_gain, wq, wk, wv, wo):
    frame_states = vit_states[frame_slot]

    def encode(operands):
        states, patches = operands
        pooled = vit_frame(states, patches, vit_ln_gain, vit_ln_bias, vit_qkv_w, vit_qkv_b, vit_out_w, vit_out_b)
        return (jnp.dot(pooled, proj_w, preferred_element_type=jnp.float32) + proj_b).astype(jnp.bfloat16)
    visual = lax.map(encode, (frame_states, patch_count))
    sequence_length = TOK_OWN * DEVICES
    positions = jnp.arange(sequence_length).astype(jnp.int32)
    token_frame = positions // TOK_OWN
    within = positions - vis_start[token_frame]
    is_visual = (within >= 0) & (within < patch_count[token_frame] // 4)
    within_clip = jnp.clip(within, 0, VIS_MAX - 1)
    visual_rows = visual[token_frame, within_clip]
    merged = jnp.where(is_visual[:, None], visual_rows, text_embed.reshape(sequence_length, MODEL_WIDTH))
    merged_wide = merged.astype(jnp.float32)
    normed_states = (merged_wide * lax.rsqrt(lax.optimization_barrier(jnp.mean(merged_wide * merged_wide, axis=1, keepdims=True)) + norm_epsilon) * attn_gain).astype(jnp.bfloat16)
    rotary_angles = rope_angles(positions, HEAD_WIDTH)[:, None, :]
    query_matrix = apply_rotary(jnp.dot(normed_states, wq, preferred_element_type=jnp.float32).reshape(sequence_length, QUERY_HEADS_HALF, HEAD_WIDTH), rotary_angles).astype(jnp.bfloat16)
    keys_complete = apply_rotary(jnp.dot(normed_states, wk, preferred_element_type=jnp.float32).reshape(sequence_length, KEY_VALUE_HEADS, HEAD_WIDTH), rotary_angles).astype(jnp.bfloat16)
    values_complete = jnp.dot(normed_states, wv, preferred_element_type=jnp.float32).astype(jnp.bfloat16).reshape(sequence_length, KEY_VALUE_HEADS, HEAD_WIDTH)
    keys_wide = keys_complete.astype(jnp.float32)
    values_wide = values_complete.astype(jnp.float32)
    grouped_rows = query_matrix.reshape(sequence_length, KEY_VALUE_HEADS, QUERY_HEADS_HALF // KEY_VALUE_HEADS, HEAD_WIDTH)
    query_rows = 128

    def attend(block_index):
        offset = block_index * query_rows
        query_block = lax.dynamic_slice_in_dim(grouped_rows, offset, query_rows, 0).astype(jnp.float32)
        scores = jnp.einsum('qkgd,nkd->kgqn', query_block, keys_wide) / math.sqrt(HEAD_WIDTH)
        query_positions = offset + jnp.arange(query_rows).astype(jnp.int32)
        allowed = positions[None, :] <= query_positions[:, None]
        scores = jnp.where(allowed[None, None], scores, masked_score)
        highest = lax.optimization_barrier(jnp.max(scores, axis=-1, keepdims=True))
        weights = jnp.where(allowed[None, None], jnp.exp(scores - highest), 0.0)
        denominator = lax.optimization_barrier(jnp.sum(weights, axis=-1))
        numerator = jnp.einsum('kgqn,nkd->kgqd', weights.astype(jnp.bfloat16).astype(jnp.float32), values_wide)
        context_block = (numerator / denominator[..., None]).astype(jnp.bfloat16)
        return jnp.transpose(context_block, (2, 0, 1, 3)).reshape(query_rows, QUERY_HEADS_HALF * HEAD_WIDTH)
    context = lax.map(attend, jnp.arange(sequence_length // query_rows).astype(jnp.int32)).reshape(sequence_length, QUERY_HEADS_HALF * HEAD_WIDTH)
    group_width = QUERY_HEADS_HALF * HEAD_WIDTH // N_FRAME
    summed = jnp.zeros((sequence_length, MODEL_WIDTH), jnp.float32)
    for head_group in range(N_FRAME):
        columns = context[:, head_group * group_width:(head_group + 1) * group_width]
        partial_sum = jnp.dot(columns, wo[head_group * group_width:(head_group + 1) * group_width], preferred_element_type=jnp.float32)
        rounded = lax.optimization_barrier(partial_sum.astype(jnp.bfloat16))
        summed = summed + rounded.astype(jnp.float32)
    return summed.astype(jnp.bfloat16).reshape(TOK_OWN, DEVICES, MODEL_WIDTH)
```

```python
import functools
import math

import jax
import jax.numpy as jnp
from jax import lax
from jax.experimental import pallas as pl
from jax.experimental.pallas import tpu as pltpu
from jax.sharding import PartitionSpec as P

MESH = pl.DeviceIdType.MESH
BF = jnp.bfloat16
F32 = jnp.float32
NEG = -1e30
ROPE_THETA = 500000.0
NEAR_FIRST = (1, 3, 2)


def remote(src, dst, send, recv, f, s):
    return pltpu.make_async_remote_copy(
        src_ref=src,
        dst_ref=dst,
        send_sem=send,
        recv_sem=recv,
        device_id={"frame": f, "seq": s},
        device_id_type=MESH,
    )


def places():
    f = lax.axis_index("frame")
    s = lax.axis_index("seq")
    y, z = s // 4, s % 4

    def along_y(k):
        return (y + k) % 4 * 4 + z

    def along_z(k):
        return y * 4 + (z + k) % 4

    def along_x(k):
        return (f // 2 + k) % 4 * 2 + f % 2

    partner = f + 1 - 2 * (f % 2)
    return f, s, along_x, along_y, along_z, partner


def greet(peers):
    barrier = pltpu.get_barrier_semaphore()
    for f, s in peers:
        pl.semaphore_signal(
            barrier, inc=1, device_id={"frame": f, "seq": s}, device_id_type=MESH
        )
    pl.semaphore_wait(barrier, len(peers))


def gather_kernel(w, t, v, wg, tg, vg, local, wss, wrs, tss, trs, vss, vrs):
    f, s, xs, ys, zs, fp = places()
    greet(
        [(f, ys(k)) for k in (1, 2, 3)]
        + [(f, zs(k)) for k in (1, 2, 3)]
        + [(xs(k), s) for k in (1, 2, 3)]
        + [(fp, s)]
    )
    sends = []

    def go(copy):
        copy.start()
        sends.append(copy)

    for i, k in enumerate(NEAR_FIRST):
        go(remote(w.at[0], wg.at[0, s], wss.at[0, 0, i], wrs.at[0, k, 0], f, ys(k)))
        go(remote(w.at[1], wg.at[1, s], wss.at[1, 0, i], wrs.at[1, k, 0], f, zs(k)))
    go(remote(v, vg.at[f % 2], vss, vrs, fp, s))
    for i, k in enumerate(NEAR_FIRST):
        go(remote(t, tg.at[f], tss.at[0, i], trs.at[0, k], xs(k), s))
    go(remote(t, tg.at[f], tss.at[1, 0], trs.at[1, 0], fp, s))
    for i, k in enumerate(NEAR_FIRST):
        go(remote(w.at[0], wg.at[0, s], wss.at[0, 1, i], wrs.at[0, 0, k], f, zs(k)))
        go(remote(w.at[1], wg.at[1, s], wss.at[1, 1, i], wrs.at[1, 0, k], f, ys(k)))
    own = [
        pltpu.make_async_copy(w.at[0], wg.at[0, s], local.at[0]),
        pltpu.make_async_copy(w.at[1], wg.at[1, s], local.at[1]),
        pltpu.make_async_copy(t, tg.at[f], local.at[2]),
        pltpu.make_async_copy(v, vg.at[f % 2], local.at[3]),
    ]
    for copy in own:
        copy.start()

    def landed(dst, recv):
        remote(dst, dst, vss, recv, fp, s).wait_recv()

    for j in NEAR_FIRST:
        a, b = ys(4 - j), zs(4 - j)
        landed(wg.at[0, a], wrs.at[0, j, 0])
        for i, k in enumerate(NEAR_FIRST):
            go(remote(wg.at[0, a], wg.at[0, a], wss.at[0, 1 + j, i], wrs.at[0, j, k], f, zs(k)))
        landed(wg.at[1, b], wrs.at[1, j, 0])
        for i, k in enumerate(NEAR_FIRST):
            go(remote(wg.at[1, b], wg.at[1, b], wss.at[1, 1 + j, i], wrs.at[1, j, k], f, ys(k)))
    for j in NEAR_FIRST:
        fs = xs(4 - j)
        landed(tg.at[fs], trs.at[0, j])
        go(remote(tg.at[fs], tg.at[fs], tss.at[1, j], trs.at[1, j], fp, s))
    for j in range(4):
        landed(tg.at[(f // 2 + 4 - j) % 4 * 2 + 1 - f % 2], trs.at[1, j])
    landed(vg.at[fp % 2], vrs)
    for j in range(4):
        for k in (1, 2, 3):
            a = ys(4 - j) // 4 * 4 + zs(4 - k) % 4
            b = ys(4 - k) // 4 * 4 + zs(4 - j) % 4
            landed(wg.at[0, a], wrs.at[0, j, k])
            landed(wg.at[1, b], wrs.at[1, j, k])
    for copy in sends:
        copy.wait_send()
    for copy in own:
        copy.wait()


def gather_inputs(w, t, v):
    shape = jax.ShapeDtypeStruct
    dma = pltpu.SemaphoreType.DMA
    return pl.pallas_call(
        gather_kernel,
        out_shape=(
            shape((2, 16) + w.shape[1:], BF),
            shape((8,) + t.shape, BF),
            shape((2,) + v.shape, BF),
        ),
        in_specs=[pl.BlockSpec(memory_space=pltpu.VMEM)] * 3,
        out_specs=(pl.BlockSpec(memory_space=pl.ANY),) * 3,
        scratch_shapes=[
            dma((4,)),
            dma((2, 5, 3)),
            dma((2, 4, 4)),
            dma((2, 4)),
            dma((2, 4)),
            dma,
            dma,
        ],
        compiler_params=pltpu.CompilerParams(
            collective_id=1, has_side_effects=True, vmem_limit_bytes=16 << 20
        ),
        cost_estimate=pl.CostEstimate(flops=0, bytes_accessed=150_000_000, transcendentals=0),
        name="gather_inputs",
    )(w, t, v)


def vision_kernel(pick, count, slots, wa, wb, gain, bias, bqk, bv, ctx, half, st, nrm, qk, vv, sem):
    core = lax.axis_index("frame") % 2
    copies = [
        pltpu.make_async_copy(slots.at[pick[a]], st.at[pl.ds(a * 256, 256)], sem.at[a])
        for a in range(2)
    ]
    for copy in copies:
        copy.start()
    for copy in copies:
        copy.wait()
    x = st[...].astype(F32)
    centred = x - jnp.mean(x, axis=1, keepdims=True)
    spread = jnp.mean(centred * centred, axis=1, keepdims=True)
    nrm[...] = (centred * lax.rsqrt(spread + 1e-6) * gain[...] + bias[...]).astype(BF)
    half[...] = st[:, pl.ds(pl.multiple_of(core * 640, 128), 640)]

    def project(i, carry):
        rows = pl.ds(pl.multiple_of(i * 128, 128), 128)
        n = nrm[rows, :]
        qk[rows, :] = (jnp.dot(n, wa[...], preferred_element_type=F32) + bqk[...]).astype(BF)
        vv[rows, :] = (jnp.dot(n, wb[...], preferred_element_type=F32) + bv[...]).astype(BF)
        return carry

    lax.fori_loop(0, 4, project, 0)
    for a in range(2):
        live = lax.broadcasted_iota(jnp.int32, (1, 256), 1) < count[a]
        rows = slice(a * 256, a * 256 + 256)
        for h in range(8):
            q = qk[rows, h * 80 : h * 80 + 80]
            k = qk[rows, 640 + h * 80 : 640 + h * 80 + 80]
            v = vv[rows, h * 80 : h * 80 + 80]
            scores = lax.dot_general(
                q, k, (((1,), (1,)), ((), ())), preferred_element_type=F32
            ) * (1.0 / math.sqrt(80))
            scores = jnp.where(live, scores, NEG)
            weights = jnp.exp(scores - jnp.max(scores, axis=1, keepdims=True))
            prob = (weights / jnp.sum(weights, axis=1, keepdims=True)).astype(BF)
            ctx[rows, h * 80 : h * 80 + 80] = jnp.dot(
                prob, v, preferred_element_type=F32
            ).astype(BF)


def vision(pick, count, slots, wa, wb, gain, bias, bqk, bv):
    shape = jax.ShapeDtypeStruct
    smem = pl.BlockSpec(memory_space=pltpu.SMEM)
    vmem = pl.BlockSpec(memory_space=pltpu.VMEM)
    return pl.pallas_call(
        vision_kernel,
        out_shape=(shape((512, 640), BF), shape((512, 640), BF)),
        in_specs=[smem, smem, pl.BlockSpec(memory_space=pl.ANY)] + [vmem] * 6,
        out_specs=(vmem, vmem),
        scratch_shapes=[
            pltpu.VMEM((512, 1280), BF),
            pltpu.VMEM((512, 1280), BF),
            pltpu.VMEM((512, 1280), BF),
            pltpu.VMEM((512, 640), BF),
            pltpu.SemaphoreType.DMA((2,)),
        ],
        compiler_params=pltpu.CompilerParams(vmem_limit_bytes=32 << 20),
        cost_estimate=pl.CostEstimate(
            flops=2_900_000_000, bytes_accessed=9_000_000, transcendentals=1_100_000
        ),
        name="vision",
    )(pick, count, slots, wa, wb, gain, bias, bqk, bv)


def token_kernel(tok, out, local, sss, srs, xss, xrs, pss, prs, land):
    f, s, xs, ys, zs, fp = places()

    def seq_at(k):
        return (s + k) % 16

    greet(
        [(f, seq_at(k)) for k in range(1, 16)] + [(xs(k), s) for k in (1, 2, 3)] + [(fp, s)]
    )
    sends = []

    def go(copy):
        copy.start()
        sends.append(copy)

    for k in range(1, 16):
        go(remote(tok.at[seq_at(k)], land.at[s], sss.at[k], srs.at[k], f, seq_at(k)))
    own = pltpu.make_async_copy(tok.at[s], land.at[s], local.at[0])
    own.start()
    own.wait()

    def landed(dst, recv):
        remote(dst, dst, sss.at[0], recv, fp, s).wait_recv()

    for k in range(1, 16):
        landed(land.at[seq_at(16 - k)], srs.at[k])
    mine = pltpu.make_async_copy(land, out.at[f], local.at[1])
    mine.start()
    for i, k in enumerate(NEAR_FIRST):
        go(remote(land, out.at[f], xss.at[i], xrs.at[k], xs(k), s))
    go(remote(land, out.at[f], pss.at[0], prs.at[0], fp, s))
    for j in NEAR_FIRST:
        fs = xs(4 - j)
        landed(out.at[fs], xrs.at[j])
        go(remote(out.at[fs], out.at[fs], pss.at[j], prs.at[j], fp, s))
    for j in range(4):
        landed(out.at[(f // 2 + 4 - j) % 4 * 2 + 1 - f % 2], prs.at[j])
    for copy in sends:
        copy.wait_send()
    mine.wait()


def exchange_tokens(tok):
    dma = pltpu.SemaphoreType.DMA
    vmem = pl.BlockSpec(memory_space=pltpu.VMEM)
    return pl.pallas_call(
        token_kernel,
        out_shape=jax.ShapeDtypeStruct((8,) + tok.shape, BF),
        in_specs=[vmem],
        out_specs=vmem,
        scratch_shapes=[
            dma((2,)),
            dma((16,)),
            dma((16,)),
            dma((3,)),
            dma((4,)),
            dma((4,)),
            dma((4,)),
            pltpu.VMEM(tok.shape, BF),
        ],
        compiler_params=pltpu.CompilerParams(
            collective_id=2, has_side_effects=True, vmem_limit_bytes=16 << 20
        ),
        cost_estimate=pl.CostEstimate(flops=0, bytes_accessed=50_000_000, transcendentals=0),
        name="exchange_tokens",
    )(tok)


def attend(q_ref, acc, top, den, kv, tile, keys, base, inc):
    scores = lax.dot_general(
        q_ref[tile], kv[:keys, :128], (((1,), (1,)), ((), ())), preferred_element_type=F32
    )
    if base is not None:
        row = lax.broadcasted_iota(jnp.int32, (512, 1), 0) % 256
        col = lax.broadcasted_iota(jnp.int32, (1, keys), 1)
        row = row % 32 * 8 + row // 32 + base + inc
        col = col // 256 * 256 + col % 32 * 8 + col % 256 // 32
        scores = jnp.where(col < row, scores, NEG)
    old = top[tile]
    new = jnp.maximum(old, jnp.max(scores, axis=1, keepdims=True))
    fade = jnp.exp2(old - new)
    weights = jnp.exp2(scores - new[:, :1]).astype(BF)
    top[tile] = new
    wide = jnp.concatenate([kv[:keys, 128:], jnp.ones((keys, 128), BF)], axis=1)
    added = jnp.dot(weights, wide, preferred_element_type=F32)
    den[tile] = den[tile] * fade + added[:, 128:]
    acc[tile] = acc[tile] * fade + added[:, :128]


def by_distance(i):
    return i + i // 2 - i // 3 * 2


def attention_kernel(q, own, out, kv, acc, top, den, ctx, local, ss, fs, rs, css, crs):
    f, s, xs, ys, zs, fp = places()
    y, z = s // 4, s % 4
    greet(
        [(f, ys(k)) for k in (1, 2, 3)]
        + [(f, zs(k)) for k in (1, 2, 3)]
        + [(xs(k), s) for k in (1, 2, 3)]
    )
    sends = []

    def go(copy):
        copy.start()
        sends.append(copy)

    for i, k in enumerate(NEAR_FIRST):
        go(remote(own.at[0], kv.at[0, s], ss.at[0, 0, i], rs.at[0, k, 0], f, ys(k)))
        go(remote(own.at[1], kv.at[1, s], ss.at[1, 0, i], rs.at[1, k, 0], f, zs(k)))
    for i, k in enumerate(NEAR_FIRST):
        go(remote(own.at[0], kv.at[0, s], ss.at[0, 1, i], rs.at[0, 0, k], f, zs(k)))
        go(remote(own.at[1], kv.at[1, s], ss.at[1, 1, i], rs.at[1, 0, k], f, ys(k)))
    kv[0, s] = own[0]
    kv[1, s] = own[1]
    top[...] = jnp.full_like(top, NEG)
    den[...] = jnp.zeros_like(den)
    acc[...] = jnp.zeros_like(acc)

    def step(i, carry):
        j = by_distance(jnp.where(i < 4, i, (i - 4) // 3))
        k = by_distance(jnp.where(i < 4, 0, (i - 4) % 3 + 1))
        a = (y + 4 - j) % 4 * 4 + (z + 4 - k) % 4
        b = (y + 4 - k) % 4 * 4 + (z + 4 - j) % 4

        @pl.when(i > 0)
        def _():
            remote(kv.at[0, a], kv.at[0, a], ss.at[0, 0, 0], rs.at[0, j, k], f, s).wait_recv()
            remote(kv.at[1, b], kv.at[1, b], ss.at[0, 0, 0], rs.at[1, j, k], f, s).wait_recv()

        @pl.when((i > 0) & (i < 4))
        def _():
            for n, d in enumerate(NEAR_FIRST):
                remote(
                    kv.at[0, a], kv.at[0, a], fs.at[0, j, n], rs.at[0, j, d], f, zs(d)
                ).start()
                remote(
                    kv.at[1, b], kv.at[1, b], fs.at[1, j, n], rs.at[1, j, d], f, ys(d)
                ).start()

        at = functools.partial(attend, q, acc, top, den)
        inc = jnp.where(a <= s, 1, 0)
        at(kv.at[0, a], 0, 256, 0, inc)
        at(kv.at[0, a], 1, 512, 256, inc)
        at(kv.at[0, a], 2, 512, None, inc)
        at(kv.at[0, a], 3, 512, None, inc)
        inc = jnp.where(b <= s, 1, 0)
        at(kv.at[1, b], 2, 256, 0, inc)
        at(kv.at[1, b], 3, 512, 256, inc)
        return carry

    lax.fori_loop(0, 16, step, 0)
    for tile in range(4):
        block = (acc[tile] / den[tile]).astype(BF)
        for head in range(2):
            for owner in range(8):
                start = head * 256 + owner * 32
                ctx[owner // 2, owner % 2, tile, head] = block[start : start + 32]
    for copy in sends:
        copy.wait_send()

    def drain(j, carry):
        for n in range(3):
            for h in range(2):
                remote(own.at[0], kv.at[0, s], fs.at[h, j, n], rs.at[0, 0, 0], f, s).wait_send()
        return carry

    lax.fori_loop(1, 4, drain, 0)
    x = f // 2
    last = []
    for i, k in enumerate(NEAR_FIRST):
        copy = remote(ctx.at[(x + k) % 4], out.at[x], css.at[i], crs.at[k], xs(k), s)
        copy.start()
        last.append(copy)
    keep = pltpu.make_async_copy(ctx.at[x], out.at[x], local)
    keep.start()
    for k in (1, 2, 3):
        here = out.at[(x + 4 - k) % 4]
        remote(here, here, css.at[0], crs.at[k], f, s).wait_recv()
    for copy in last:
        copy.wait_send()
    keep.wait()


def attention(q, own):
    dma = pltpu.SemaphoreType.DMA
    vmem = pl.BlockSpec(memory_space=pltpu.VMEM)
    state = pltpu.VMEM((4, 512, 128), F32)
    return pl.pallas_call(
        attention_kernel,
        out_shape=jax.ShapeDtypeStruct((4, 2, 4, 2, 32, 128), BF),
        in_specs=[vmem, vmem],
        out_specs=vmem,
        scratch_shapes=[
            pltpu.VMEM((2, 16, 512, 256), BF),
            state,
            state,
            state,
            pltpu.VMEM((4, 2, 4, 2, 32, 128), BF),
            dma,
            dma((2, 2, 3)),
            dma((2, 4, 3)),
            dma((2, 4, 4)),
            dma((3,)),
            dma((4,)),
        ],
        compiler_params=pltpu.CompilerParams(
            collective_id=3, has_side_effects=True, vmem_limit_bytes=40 << 20
        ),
        cost_estimate=pl.CostEstimate(
            flops=24_000_000_000, bytes_accessed=9_000_000, transcendentals=20_000_000
        ),
        name="attention",
    )(q, own)


def swap_cores(value):
    return lax.ppermute(value, "frame", [(i, i ^ 1) for i in range(8)])


def per_device(
    vit_states,
    frame_slot,
    patch_count,
    vis_start,
    text_embed,
    vit_ln_gain,
    vit_ln_bias,
    vit_qkv_w,
    vit_qkv_b,
    vit_out_w,
    vit_out_b,
    proj_w,
    proj_b,
    attn_gain,
    wq,
    wk,
    wv,
    wo,
):
    f = lax.axis_index("frame")
    s = lax.axis_index("seq")
    core = f % 2
    holder = frame_slot // 2
    pair = holder // 32 * 16 + holder % 16
    order = holder // 16 % 2 * 2 + frame_slot % 2
    before = (pair[:, None] == pair[None, :]) & (order[None, :] < order[:, None])
    rank = jnp.sum(before.astype(jnp.int32), axis=1)
    here = (pair == f // 2 * 16 + s)[None, :] & (rank[None, :] == jnp.arange(2)[:, None])
    facts = jnp.stack([order, patch_count, vis_start])
    facts = jnp.sum(jnp.where(here[None], facts[:, None, :], 0), axis=2)
    pick, count, start = facts[0], facts[1], facts[2]

    def half_of(a):
        return jnp.where(core == 0, a[..., :640], a[..., 640:])

    qw, kw, vw = jnp.split(vit_qkv_w, 3, axis=1)
    qb, kb, vb = jnp.split(vit_qkv_b, 3)
    shard = jnp.stack(
        [
            jnp.concatenate([half_of(qw), half_of(kw)], axis=1),
            jnp.concatenate([half_of(vw), half_of(vit_out_w)], axis=1),
        ]
    )
    text = text_embed.reshape(128, 4096).astype(F32)
    text = (
        text * lax.rsqrt(jnp.mean(text * text, axis=1, keepdims=True) + 1e-5) * attn_gain
    ).astype(BF)
    weights, texts, slots = gather_inputs(shard, text, vit_states)
    wo_late = lax.optimization_barrier((wo, weights))[0]
    wo_parts = [wo] + [
        lax.ppermute(wo_late, "frame", [(i, i ^ k) for i in range(8)]) for k in (2, 6, 4)
    ]
    weights = weights.reshape(2, 1280, 1280)
    ctx, states_half = vision(
        pick,
        count,
        slots.reshape(4, 256, 1280),
        weights[0],
        weights[1, :, :640],
        vit_ln_gain[None],
        vit_ln_bias[None],
        jnp.concatenate([half_of(qb), half_of(kb)])[None],
        half_of(vb)[None],
    )
    other = swap_cores(ctx)
    ctx = jnp.where(
        core == 0, jnp.concatenate([ctx, other], axis=1), jnp.concatenate([other, ctx], axis=1)
    )
    attended = jnp.dot(ctx, weights[1, :, 640:], preferred_element_type=F32)
    hidden = (states_half.astype(F32) + attended + half_of(vit_out_b)).astype(BF)
    pooled = jnp.mean(hidden.astype(F32).reshape(128, 4, 640), axis=1).astype(BF)
    other = swap_cores(pooled)
    whole = jnp.where(
        core == 0,
        jnp.concatenate([pooled, other], axis=1),
        jnp.concatenate([other, pooled], axis=1),
    )
    seen = jnp.dot(whole, proj_w, preferred_element_type=F32) + proj_b
    scale = lax.rsqrt(jnp.mean(seen * seen, axis=1, keepdims=True) + 1e-5)
    lane = jnp.arange(128)[None, :]
    tokens = jnp.concatenate(
        [(pooled.astype(F32) * scale).astype(BF), jnp.where(lane == 0, scale, 0.0).astype(BF)],
        axis=1,
    )
    want = jnp.arange(128)
    frame_of = want // 4 % 2
    token = (want // 8 - jnp.where(frame_of == 0, start[0], start[1])) % 16 + want % 4 * 16
    taken = (frame_of * 64 + token)[:, None] == jnp.arange(128)[None, :]
    tokens = jnp.dot(taken.astype(BF), tokens, preferred_element_type=F32).astype(BF)
    table = exchange_tokens(tokens.reshape(16, 8, 768)).reshape(4, 2, 128, 768)
    wide = jnp.concatenate([wq, wk, wv], axis=1)
    gained = (attn_gain[:, None] * wide.astype(F32)).astype(BF)
    folded = jnp.dot(proj_w, gained, preferred_element_type=F32).astype(BF)
    bias_high = proj_b.astype(BF)
    bias_low = (proj_b - bias_high.astype(F32)).astype(BF)
    bias = jnp.sum(
        jnp.dot(jnp.stack([bias_high, bias_low]), gained, preferred_element_type=F32),
        axis=0,
        keepdims=True,
    )
    bias = jnp.where(lane.T == 0, bias, 0.0).astype(BF)
    low = jnp.concatenate([folded[:640], bias], axis=0)
    high = jnp.concatenate([folded[640:], jnp.zeros_like(bias)], axis=0)
    visual = (
        jnp.dot(table[:, 0].reshape(512, 768), low, preferred_element_type=F32)
        + jnp.dot(table[:, 1].reshape(512, 768), high, preferred_element_type=F32)
    ).astype(BF)
    owner = jnp.arange(8)[None, :, None]
    frame = jnp.arange(128).reshape(4, 1, 32)
    within = frame * 128 + owner * 16 + s - vis_start.reshape(4, 1, 32)
    live = (within >= 0) & (within < patch_count.reshape(4, 1, 32) // 4)
    source = (pair * 8 + rank * 4).reshape(4, 1, 32) + within // 16
    source = jnp.where(live, source, -1).reshape(1024, 1)
    chosen = (source == jnp.arange(512)[None, :]).astype(BF)
    visual = jnp.dot(chosen, visual, preferred_element_type=F32)
    texts = texts.reshape(8, 4, 32, 4096).transpose(1, 0, 2, 3).reshape(1024, 4096)
    plain = jnp.dot(texts, wide, preferred_element_type=F32)
    projected = jnp.where(source >= 0, visual, plain)
    position = (frame * 128 + owner * 16 + s).reshape(1024, 1).astype(F32)
    exponents = jnp.arange(0, 128, 2).astype(F32) / 128
    angles = position * jnp.power(F32(ROPE_THETA), -exponents)[None, :]
    cosine, sine = jnp.cos(angles), jnp.sin(angles)

    def rotate(v):
        a, b = v[:, :64], v[:, 64:]
        return jnp.concatenate([a * cosine - b * sine, b * cosine + a * sine], axis=1)

    factor = math.log2(math.e) / math.sqrt(128)
    queries = jnp.stack(
        [(rotate(projected[:, h * 128 : h * 128 + 128]) * factor).astype(BF) for h in range(2)]
    )
    queries = queries.reshape(2, 4, 256, 128).transpose(1, 0, 2, 3).reshape(4, 512, 128)
    own = jnp.concatenate(
        [rotate(projected[:, 256:384]).astype(BF), projected[:, 384:].astype(BF)], axis=1
    )
    ctx = attention(queries, own.reshape(2, 512, 256))
    ctx = ctx.transpose(1, 2, 4, 0, 3, 5).reshape(256, 4, 256)
    x = f // 2
    partial = jnp.zeros((256, 4096), F32)
    for k, part in zip((0, 1, 3, 2), wo_parts):
        columns = lax.dynamic_index_in_dim(ctx, x ^ k, axis=1, keepdims=False)
        partial = partial + jnp.dot(columns, part, preferred_element_type=F32)
    keep = jnp.where(core == 0, partial[:128], partial[128:])
    give = jnp.where(core == 0, partial[128:], partial[:128]).astype(BF)
    mixed = (keep + swap_cores(give).astype(F32)).astype(BF)
    return mixed.reshape(128, 1, 4096)


def solution(mesh):
    return jax.shard_map(
        per_device,
        mesh=mesh,
        in_specs=(
            P(("frame", "seq"), None, None),
            P(),
            P(),
            P(),
            P(None, ("frame", "seq"), None),
            P(),
            P(),
            P("seq", None),
            P(),
            P("seq", None),
            P(),
            P(),
            P(),
            P(),
            P(None, "frame"),
            P(None, "frame"),
            P(None, "frame"),
            P("frame", None),
        ),
        out_specs=P(None, ("frame", "seq"), None),
        check_vma=False,
    )
```

```python
import functools
import math

import jax
import jax.numpy as jnp
from jax import lax
from jax.experimental import pallas as pl
from jax.experimental.pallas import tpu as pltpu
from jax.sharding import PartitionSpec as P

MESH = pl.DeviceIdType.MESH
BF = jnp.bfloat16
F32 = jnp.float32
NEG = -1e30
ROPE_THETA = 500000.0
NEAR_FIRST = (1, 3, 2)


def remote(src, dst, send, recv, f, s):
    return pltpu.make_async_remote_copy(
        src_ref=src,
        dst_ref=dst,
        send_sem=send,
        recv_sem=recv,
        device_id={"frame": f, "seq": s},
        device_id_type=MESH,
    )


def places():
    f = lax.axis_index("frame")
    s = lax.axis_index("seq")
    y, z = s // 4, s % 4

    def along_y(k):
        return (y + k) % 4 * 4 + z

    def along_z(k):
        return y * 4 + (z + k) % 4

    def along_x(k):
        return (f // 2 + k) % 4 * 2 + f % 2

    partner = f + 1 - 2 * (f % 2)
    return f, s, along_x, along_y, along_z, partner


def greet(peers):
    barrier = pltpu.get_barrier_semaphore()
    for f, s in peers:
        pl.semaphore_signal(
            barrier, inc=1, device_id={"frame": f, "seq": s}, device_id_type=MESH
        )
    pl.semaphore_wait(barrier, len(peers))


def turned(row, eye):
    return jnp.sum(jnp.where(eye, row.astype(F32), 0.0), axis=1, keepdims=True).astype(jnp.int32)


def front_kernel(
    slot_r, count_r, start_r, v, qkvw, outw, t, ln_g, ln_b, qkvb, outb, pbias, again, ca, sa, cb, sb, pb,
    proj, wq, wk, wv,
    q_out, kv_out,
    ws, wg, vp, tg, pw, wc, fold, plain, st, nrm, qk, vv, ctx, ctxo, pool, poolo, tok, land, table, col,
    local, wss, wrs, tss, trs, vss, vrs, ess, ers, sss, srs, xss, xrs, pss, prs,
):
    f, s, xs, ys, zs, fp = places()
    core = f % 2

    def seq_at(k):
        return (s + k) % 16

    def lanes(first):
        return pl.ds(pl.multiple_of(first + core * 640, 128), 640)

    def landed(dst, recv):
        remote(dst, dst, vss, recv, fp, s).wait_recv()

    packs = [
        pltpu.make_async_copy(qkvw.at[:, lanes(0)], ws.at[0, :, pl.ds(0, 640)], local.at[0]),
        pltpu.make_async_copy(qkvw.at[:, lanes(1280)], ws.at[0, :, pl.ds(640, 640)], local.at[1]),
        pltpu.make_async_copy(qkvw.at[:, lanes(2560)], ws.at[1, :, pl.ds(0, 640)], local.at[2]),
        pltpu.make_async_copy(outw.at[:, lanes(0)], ws.at[1, :, pl.ds(640, 640)], local.at[3]),
    ]
    loads = [
        pltpu.make_async_copy(wq, wc.at[:, pl.ds(0, 256)], local.at[4]),
        pltpu.make_async_copy(wk, wc.at[:, pl.ds(256, 128)], local.at[5]),
        pltpu.make_async_copy(wv, wc.at[:, pl.ds(384, 128)], local.at[6]),
        pltpu.make_async_copy(proj, pw, local.at[7]),
    ]
    for copy in packs:
        copy.start()
    greet(
        [(f, seq_at(k)) for k in range(1, 16)]
        + [(xs(k), s) for k in (1, 2, 3)]
        + [(fp, s)]
    )
    for copy in packs:
        copy.wait()
    sends = []

    def go(copy):
        copy.start()
        sends.append(copy)

    for i, k in enumerate(NEAR_FIRST):
        go(remote(ws.at[0], wg.at[0, s], wss.at[0, 0, i], wrs.at[0, k, 0], f, ys(k)))
        go(remote(ws.at[1], wg.at[1, s], wss.at[1, 0, i], wrs.at[1, k, 0], f, zs(k)))
    go(remote(v, vp, vss, vrs, fp, s))
    for i, k in enumerate(NEAR_FIRST):
        go(remote(t, tg.at[f], tss.at[0, i], trs.at[0, k], xs(k), s))
    go(remote(t, tg.at[f], tss.at[1, 0], trs.at[1, 0], fp, s))
    for i, k in enumerate(NEAR_FIRST):
        go(remote(ws.at[0], wg.at[0, s], wss.at[0, 1, i], wrs.at[0, 0, k], f, zs(k)))
        go(remote(ws.at[1], wg.at[1, s], wss.at[1, 1, i], wrs.at[1, 0, k], f, ys(k)))
    for copy in loads:
        copy.start()
    wg[0, s] = ws[0]
    wg[1, s] = ws[1]
    slot = slot_r[...]
    holder = slot // 2
    pair = holder // 32 * 16 + holder % 16
    order = holder // 16 % 2 * 2 + slot % 2
    eye = lax.broadcasted_iota(jnp.int32, (128, 128), 0) == lax.broadcasted_iota(
        jnp.int32, (128, 128), 1
    )
    pair_c, order_c = turned(pair, eye), turned(order, eye)
    same = pair_c == pair
    rank = jnp.sum(jnp.where(same & (order_c < order), 1.0, 0.0), axis=0, keepdims=True).astype(
        jnp.int32
    )
    col[:, 0:1] = pair_c * 8 + turned(rank, eye) * 4
    col[:, 1:2] = turned(start_r[...], eye)
    col[:, 2:3] = turned(count_r[...], eye)
    facts = []
    for a in range(2):
        mine = (pair == f // 2 * 16 + s) & (rank == a)
        facts.append(
            [
                jnp.sum(
                    jnp.where(mine, row.astype(F32), 0.0), axis=1, keepdims=True
                ).astype(jnp.int32)
                for row in (order, count_r[...], start_r[...])
            ]
        )
    for copy in loads:
        copy.wait()

    def fold_rows(i, carry):
        rows = pl.ds(pl.multiple_of(i * 128, 128), 128)
        to = pl.ds(pl.multiple_of(i * 128 + i // 5 * 128, 128), 128)
        gained = (pw[rows, :].astype(F32) * again[...]).astype(BF)
        fold[to, :] = jnp.dot(gained, wc[...], preferred_element_type=F32).astype(BF)
        return carry

    def text_rows(source, at):
        plain[:, at] = jnp.dot(source[...], wc[...], preferred_element_type=F32).reshape(4, 32, 512)

    def forward_weights(j):
        a, b = ys(4 - j), zs(4 - j)
        landed(wg.at[0, a], wrs.at[0, j, 0])
        for i, k in enumerate(NEAR_FIRST):
            go(remote(wg.at[0, a], wg.at[0, a], wss.at[0, 1 + j, i], wrs.at[0, j, k], f, zs(k)))
        landed(wg.at[1, b], wrs.at[1, j, 0])
        for i, k in enumerate(NEAR_FIRST):
            go(remote(wg.at[1, b], wg.at[1, b], wss.at[1, 1 + j, i], wrs.at[1, j, k], f, ys(k)))

    lax.fori_loop(0, 2, fold_rows, 0)
    forward_weights(1)
    forward_weights(3)
    lax.fori_loop(2, 5, fold_rows, 0)
    forward_weights(2)
    lax.fori_loop(5, 10, fold_rows, 0)
    biased = jnp.dot(pbias[...], wc[...], preferred_element_type=F32)
    biased = jnp.sum(biased, axis=0, keepdims=True)
    first = lax.broadcasted_iota(jnp.int32, (128, 512), 0) == 0
    fold[640:768, :] = jnp.where(first, biased, 0.0).astype(BF)
    fold[1408:1536, :] = jnp.zeros((128, 512), BF)
    text_rows(t, f)
    landed(vp, vrs)
    for a in range(2):
        pick = facts[a][0]
        chosen = jnp.zeros((256, 1280), F32)
        for n in range(2):
            chosen = jnp.where(pick == core * 2 + n, v[n].astype(F32), chosen)
            chosen = jnp.where(pick == 2 - core * 2 + n, vp[n].astype(F32), chosen)
        st[a * 256 : a * 256 + 256, :] = chosen.astype(BF)

    def norm_rows(i, carry):
        rows = pl.ds(pl.multiple_of(i * 128, 128), 128)
        x = st[rows, :].astype(F32)
        centred = x - jnp.mean(x, axis=1, keepdims=True)
        spread = jnp.mean(centred * centred, axis=1, keepdims=True)
        nrm[rows, :] = (centred * lax.rsqrt(spread + 1e-6) * ln_g[...] + ln_b[...]).astype(BF)
        return carry

    lax.fori_loop(0, 4, norm_rows, 0)
    for j in NEAR_FIRST:
        fs = xs(4 - j)
        landed(tg.at[fs], trs.at[0, j])
        go(remote(tg.at[fs], tg.at[fs], tss.at[1, j], trs.at[1, j], fp, s))
        text_rows(tg.at[fs], fs)
    for j in (0, 1, 3, 2):
        fs = (f // 2 + 4 - j) % 4 * 2 + 1 - core
        landed(tg.at[fs], trs.at[1, j])
        text_rows(tg.at[fs], fs)
    for j in range(4):
        for k in (1, 2, 3):
            a = ys(4 - j) // 4 * 4 + zs(4 - k) % 4
            b = ys(4 - k) // 4 * 4 + zs(4 - j) % 4
            landed(wg.at[0, a], wrs.at[0, j, k])
            landed(wg.at[1, b], wrs.at[1, j, k])

    def project(i, carry):
        rows = pl.ds(pl.multiple_of(i * 128, 128), 128)
        n = nrm[rows, :]
        both = jnp.dot(n, wg[0].reshape(1280, 1280), preferred_element_type=F32)
        qk[rows, :640] = (both[:, :640] + qkvb[:, lanes(0)]).astype(BF)
        qk[rows, 640:] = (both[:, 640:] + qkvb[:, lanes(1280)]).astype(BF)
        third = jnp.dot(n, wg[1, :, :, :640].reshape(1280, 640), preferred_element_type=F32)
        vv[rows, :] = (third + qkvb[:, lanes(2560)]).astype(BF)
        return carry

    lax.fori_loop(0, 4, project, 0)
    for a in range(2):
        live = lax.broadcasted_iota(jnp.int32, (1, 256), 1) < facts[a][1]
        rows = slice(a * 256, a * 256 + 256)
        for h in range(8):
            q = qk[rows, h * 80 : h * 80 + 80]
            k = qk[rows, 640 + h * 80 : 640 + h * 80 + 80]
            val = vv[rows, h * 80 : h * 80 + 80]
            scores = lax.dot_general(
                q, k, (((1,), (1,)), ((), ())), preferred_element_type=F32
            ) * (1.0 / math.sqrt(80))
            scores = jnp.where(live, scores, NEG)
            weights = jnp.exp(scores - jnp.max(scores, axis=1, keepdims=True))
            prob = (weights / jnp.sum(weights, axis=1, keepdims=True)).astype(BF)
            ctx[rows, h * 80 : h * 80 + 80] = jnp.dot(
                prob, val, preferred_element_type=F32
            ).astype(BF)
    go(remote(ctx, ctxo, ess.at[0], ers.at[0], fp, s))

    def out_rows(owner):
        return wg[1, pl.ds(owner * 8, 8), :, 640:].reshape(640, 640)

    attended = jnp.dot(ctx[...], out_rows(core), preferred_element_type=F32)
    landed(ctxo, ers.at[0])
    attended = attended + jnp.dot(ctxo[...], out_rows(1 - core), preferred_element_type=F32)
    hidden = (st[:, lanes(0)].astype(F32) + attended + outb[:, lanes(0)]).astype(BF)
    quarter = lax.broadcasted_iota(jnp.int32, (128, 512), 1) // 4 == lax.broadcasted_iota(
        jnp.int32, (128, 512), 0
    )
    pooled = jnp.dot(
        jnp.where(quarter, 0.25, 0.0).astype(BF), hidden, preferred_element_type=F32
    )
    pool[...] = pooled.astype(BF)
    go(remote(pool, poolo, ess.at[1], ers.at[1], fp, s))
    landed(poolo, ers.at[1])

    def square(c, total):
        cols = pl.ds(pl.multiple_of(c * 512, 128), 512)
        own_rows = pl.ds(pl.multiple_of(core * 640, 128), 640)
        other_rows = pl.ds(pl.multiple_of(640 - core * 640, 128), 640)
        seen = jnp.dot(pool[...], pw[own_rows, cols], preferred_element_type=F32)
        seen = seen + jnp.dot(poolo[...], pw[other_rows, cols], preferred_element_type=F32)
        seen = seen + pb[:, cols]
        return total + jnp.sum(seen * seen, axis=1, keepdims=True)

    total = lax.fori_loop(0, 8, square, jnp.zeros((128, 1), F32))
    scale = lax.rsqrt(total * (1.0 / 4096) + 1e-5)
    head = (pool[...].astype(F32) * scale).astype(BF)
    tail = jnp.where(lax.broadcasted_iota(jnp.int32, (128, 128), 1) == 0, scale, 0.0).astype(BF)
    want = lax.broadcasted_iota(jnp.int32, (128, 1), 0)
    frame_of = want // 4 % 2
    begin = jnp.where(frame_of == 0, facts[0][2], facts[1][2])
    token = (want // 8 - begin + 16384) % 16 + want % 4 * 16 + frame_of * 64
    taken = (token == lax.broadcasted_iota(jnp.int32, (128, 128), 1)).astype(F32).astype(BF)
    head = jnp.dot(taken, head, preferred_element_type=F32)
    tail = jnp.dot(taken, tail, preferred_element_type=F32)
    for i in range(16):
        tok[i, :, :640] = head[i * 8 : i * 8 + 8].astype(BF)
        tok[i, :, 640:] = tail[i * 8 : i * 8 + 8].astype(BF)
    for k in range(1, 16):
        go(remote(tok.at[seq_at(k)], land.at[s], sss.at[k], srs.at[k], f, seq_at(k)))
    land[s] = tok[s]
    for k in range(1, 16):
        landed(land.at[seq_at(16 - k)], srs.at[k])
    for i, k in enumerate(NEAR_FIRST):
        go(remote(land, table.at[f], xss.at[i], xrs.at[k], xs(k), s))
    go(remote(land, table.at[f], pss.at[0], prs.at[0], fp, s))
    table[f] = land[...]
    for j in NEAR_FIRST:
        fs = xs(4 - j)
        landed(table.at[fs], xrs.at[j])
        go(remote(table.at[fs], table.at[fs], pss.at[j], prs.at[j], fp, s))
    for j in range(4):
        landed(table.at[(f // 2 + 4 - j) % 4 * 2 + 1 - core], prs.at[j])
    parts = []
    for x in range(4):
        even = table[2 * x].astype(F32).reshape(128, 768).astype(BF)
        odd = table[2 * x + 1].astype(F32).reshape(128, 768).astype(BF)
        part = jnp.dot(even, fold[:768, :], preferred_element_type=F32)
        part = part + jnp.dot(odd, fold[768:, :], preferred_element_type=F32)
        parts.append(part.astype(BF))
    visual = jnp.concatenate(parts, axis=0)
    sign = jnp.where(lax.broadcasted_iota(jnp.int32, (1, 128), 1) < 64, -1.0, 1.0)
    factor = math.log2(math.e) / math.sqrt(128)
    for blk in range(4):
        some = slice(blk * 32, blk * 32 + 32)
        shape = (8, 32, 1)
        frame = lax.broadcasted_iota(jnp.int32, shape, 1) + blk * 32
        owner = lax.broadcasted_iota(jnp.int32, shape, 0)
        within = frame * 128 + owner * 16 + s - col[some, 1:2][None]
        live = (within >= 0) & (within < col[some, 2:3][None] // 4)
        source = jnp.where(live, col[some, 0:1][None] + within // 16, -1).reshape(256, 1)
        chosen = (source == lax.broadcasted_iota(jnp.int32, (256, 512), 1)).astype(F32).astype(BF)
        placed = jnp.dot(chosen, visual, preferred_element_type=F32)
        x = jnp.where(source >= 0, placed, plain[blk].reshape(256, 512))
        c1, s1 = ca[some, :][None], sa[some, :][None]
        c2, s2 = cb[...][:, None, :], sb[...][:, None, :]
        cosine = (c1 * c2 - s1 * s2).reshape(256, 128)
        sine = (s1 * c2 + c1 * s2).reshape(256, 128) * sign

        def rotate(n):
            part = x[:, n * 128 : n * 128 + 128]
            return part * cosine + pltpu.roll(part, 64, 1) * sine

        for h in range(2):
            q_out[blk, h * 256 : h * 256 + 256, :] = (rotate(h) * factor).astype(BF)
        rows = slice(blk % 2 * 256, blk % 2 * 256 + 256)
        kv_out[blk // 2, rows, :128] = rotate(2).astype(BF)
        kv_out[blk // 2, rows, 128:] = x[:, 384:].astype(BF)
    for copy in sends:
        copy.wait_send()


def front(rows, vmem_args, hbm_args):
    shape = jax.ShapeDtypeStruct
    dma = pltpu.SemaphoreType.DMA
    vmem = pl.BlockSpec(memory_space=pltpu.VMEM)
    hbm = pl.BlockSpec(memory_space=pl.ANY)
    buf = pltpu.VMEM
    return pl.pallas_call(
        front_kernel,
        out_shape=(shape((4, 512, 128), BF), shape((2, 512, 256), BF)),
        in_specs=[vmem] * (len(rows) + len(vmem_args)) + [hbm] * len(hbm_args),
        out_specs=(vmem, vmem),
        scratch_shapes=[
            buf((2, 80, 1280), BF),
            buf((2, 16, 80, 1280), BF),
            buf((2, 256, 1280), BF),
            buf((8, 128, 4096), BF),
            buf((1280, 4096), BF),
            buf((4096, 512), BF),
            buf((1536, 512), BF),
            buf((4, 8, 32, 512), F32),
            buf((512, 1280), BF),
            buf((512, 1280), BF),
            buf((512, 1280), BF),
            buf((512, 640), BF),
            buf((512, 640), BF),
            buf((512, 640), BF),
            buf((128, 640), BF),
            buf((128, 640), BF),
            buf((16, 8, 768), BF),
            buf((16, 8, 768), BF),
            buf((8, 16, 8, 768), BF),
            buf((128, 128), jnp.int32),
            dma((8,)),
            dma((2, 5, 3)),
            dma((2, 4, 4)),
            dma((2, 4)),
            dma((2, 4)),
            dma,
            dma,
            dma((2,)),
            dma((2,)),
            dma((16,)),
            dma((16,)),
            dma((3,)),
            dma((4,)),
            dma((4,)),
            dma((4,)),
        ],
        compiler_params=pltpu.CompilerParams(
            collective_id=1, has_side_effects=True, vmem_limit_bytes=56 << 20
        ),
        name="front",
    )(*rows, *vmem_args, *hbm_args)


def attend(q_ref, acc, top, den, kv, tile, keys, base, inc):
    scores = lax.dot_general(
        q_ref[tile], kv[:keys, :128], (((1,), (1,)), ((), ())), preferred_element_type=F32
    )
    if base is not None:
        row = lax.broadcasted_iota(jnp.int32, (512, 1), 0) % 256
        col = lax.broadcasted_iota(jnp.int32, (1, keys), 1)
        row = row % 32 * 8 + row // 32 + base + inc
        col = col // 256 * 256 + col % 32 * 8 + col % 256 // 32
        scores = jnp.where(col < row, scores, NEG)
    old = top[tile]
    new = jnp.maximum(old, jnp.max(scores, axis=1, keepdims=True))
    fade = jnp.exp2(old - new)
    weights = jnp.exp2(scores - new[:, :1]).astype(BF)
    top[tile] = new
    wide = jnp.concatenate([kv[:keys, 128:], jnp.ones((keys, 128), BF)], axis=1)
    added = jnp.dot(weights, wide, preferred_element_type=F32)
    den[tile] = den[tile] * fade + added[:, 128:]
    acc[tile] = acc[tile] * fade + added[:, :128]


def by_distance(i):
    return i + i // 2 - i // 3 * 2


def attention_kernel(
    q, own, wo, out, wog, kv, acc, top, den, ctx, local, ss, fs, rs, css, crs, oss, ors
):
    f, s, xs, ys, zs, fp = places()
    y, z = s // 4, s % 4
    greet(
        [(f, ys(k)) for k in (1, 2, 3)]
        + [(f, zs(k)) for k in (1, 2, 3)]
        + [(xs(k), s) for k in (1, 2, 3)]
    )
    sends = []

    def go(copy):
        copy.start()
        sends.append(copy)

    for i, k in enumerate(NEAR_FIRST):
        go(remote(own.at[0], kv.at[0, s], ss.at[0, 0, i], rs.at[0, k, 0], f, ys(k)))
        go(remote(own.at[1], kv.at[1, s], ss.at[1, 0, i], rs.at[1, k, 0], f, zs(k)))
    for i, k in enumerate(NEAR_FIRST):
        go(remote(own.at[0], kv.at[0, s], ss.at[0, 1, i], rs.at[0, 0, k], f, zs(k)))
        go(remote(own.at[1], kv.at[1, s], ss.at[1, 1, i], rs.at[1, 0, k], f, ys(k)))
    for n in range(2):
        go(remote(wo, wog.at[1 + 2 * n], oss.at[n], ors.at[n], xs(3 - 2 * n), s))
    mine = pltpu.make_async_copy(wo, wog.at[0], local.at[1])
    mine.start()
    kv[0, s] = own[0]
    kv[1, s] = own[1]
    top[...] = jnp.full_like(top, NEG)
    den[...] = jnp.zeros_like(den)
    acc[...] = jnp.zeros_like(acc)

    def step(i, carry):
        j = by_distance(jnp.where(i < 4, i, (i - 4) // 3))
        k = by_distance(jnp.where(i < 4, 0, (i - 4) % 3 + 1))
        a = (y + 4 - j) % 4 * 4 + (z + 4 - k) % 4
        b = (y + 4 - k) % 4 * 4 + (z + 4 - j) % 4

        @pl.when(i > 0)
        def _():
            remote(kv.at[0, a], kv.at[0, a], ss.at[0, 0, 0], rs.at[0, j, k], f, s).wait_recv()
            remote(kv.at[1, b], kv.at[1, b], ss.at[0, 0, 0], rs.at[1, j, k], f, s).wait_recv()

        @pl.when((i > 0) & (i < 4))
        def _():
            for n, d in enumerate(NEAR_FIRST):
                remote(
                    kv.at[0, a], kv.at[0, a], fs.at[0, j, n], rs.at[0, j, d], f, zs(d)
                ).start()
                remote(
                    kv.at[1, b], kv.at[1, b], fs.at[1, j, n], rs.at[1, j, d], f, ys(d)
                ).start()

        @pl.when(i == 12)
        def _():
            for n in range(2):
                here = wog.at[1 + 2 * n]
                remote(here, here, oss.at[n], ors.at[n], f, s).wait_recv()
                half = pl.ds(n * 128, 128)
                remote(
                    here.at[half],
                    wog.at[2, half],
                    oss.at[2 + n],
                    ors.at[2 + n],
                    xs(3 - 2 * n),
                    s,
                ).start()

        at = functools.partial(attend, q, acc, top, den)
        inc = jnp.where(a <= s, 1, 0)
        at(kv.at[0, a], 0, 256, 0, inc)
        at(kv.at[0, a], 1, 512, 256, inc)
        at(kv.at[0, a], 2, 512, None, inc)
        at(kv.at[0, a], 3, 512, None, inc)
        inc = jnp.where(b <= s, 1, 0)
        at(kv.at[1, b], 2, 256, 0, inc)
        at(kv.at[1, b], 3, 512, 256, inc)
        return carry

    lax.fori_loop(0, 16, step, 0)
    for tile in range(4):
        block = (acc[tile] / den[tile]).astype(BF)
        for head in range(2):
            for owner in range(8):
                start = head * 256 + owner * 32
                ctx[owner // 2, owner % 2, tile, head] = block[start : start + 32]
    for copy in sends:
        copy.wait_send()

    def drain(j, carry):
        for n in range(3):
            for h in range(2):
                remote(own.at[0], kv.at[0, s], fs.at[h, j, n], rs.at[0, 0, 0], f, s).wait_send()
        return carry

    lax.fori_loop(1, 4, drain, 0)
    x = f // 2
    last = []
    for i, k in enumerate(NEAR_FIRST):
        copy = remote(ctx.at[(x + k) % 4], out.at[4 - k], css.at[i], crs.at[k], xs(k), s)
        copy.start()
        last.append(copy)
    keep = pltpu.make_async_copy(ctx.at[x], out.at[0], local.at[0])
    keep.start()
    for k in (1, 2, 3):
        here = out.at[4 - k]
        remote(here, here, css.at[0], crs.at[k], f, s).wait_recv()
    for copy in last:
        copy.wait_send()
    keep.wait()
    mine.wait()
    for n in range(2):
        half = wog.at[2, pl.ds(n * 128, 128)]
        remote(half, half, oss.at[2 + n], ors.at[2 + n], f, s).wait()


def attention(q, own, wo):
    dma = pltpu.SemaphoreType.DMA
    vmem = pl.BlockSpec(memory_space=pltpu.VMEM)
    hbm = pl.BlockSpec(memory_space=pl.ANY)
    state = pltpu.VMEM((4, 512, 128), F32)
    return pl.pallas_call(
        attention_kernel,
        out_shape=(
            jax.ShapeDtypeStruct((4, 2, 4, 2, 32, 128), BF),
            jax.ShapeDtypeStruct((4, 256, 4096), BF),
        ),
        in_specs=[vmem, vmem, hbm],
        out_specs=(vmem, hbm),
        scratch_shapes=[
            pltpu.VMEM((2, 16, 512, 256), BF),
            state,
            state,
            state,
            pltpu.VMEM((4, 2, 4, 2, 32, 128), BF),
            dma((2,)),
            dma((2, 2, 3)),
            dma((2, 4, 3)),
            dma((2, 4, 4)),
            dma((3,)),
            dma((4,)),
            dma((4,)),
            dma((4,)),
        ],
        compiler_params=pltpu.CompilerParams(
            collective_id=3, has_side_effects=True, vmem_limit_bytes=40 << 20
        ),
        cost_estimate=pl.CostEstimate(
            flops=24_000_000_000, bytes_accessed=9_000_000, transcendentals=20_000_000
        ),
        name="attention",
    )(q, own, wo)


def swap_cores(value):
    return lax.ppermute(value, "frame", [(i, i ^ 1) for i in range(8)])


def per_device(
    vit_states,
    frame_slot,
    patch_count,
    vis_start,
    text_embed,
    vit_ln_gain,
    vit_ln_bias,
    vit_qkv_w,
    vit_qkv_b,
    vit_out_w,
    vit_out_b,
    proj_w,
    proj_b,
    attn_gain,
    wq,
    wk,
    wv,
    wo,
):
    f = lax.axis_index("frame")
    s = lax.axis_index("seq")
    core = f % 2
    text = text_embed.reshape(128, 4096).astype(F32)
    text = (
        text * lax.rsqrt(jnp.mean(text * text, axis=1, keepdims=True) + 1e-5) * attn_gain
    ).astype(BF)
    gained = proj_b * attn_gain
    high = gained.astype(BF)
    low = (gained - high.astype(F32)).astype(BF)
    row = jnp.arange(16)[:, None]
    pbias = jnp.where(row == 0, high[None], jnp.where(row == 1, low[None], jnp.zeros((), BF)))
    exponents = jnp.arange(0, 128, 2).astype(F32) / 128
    inverse = jnp.power(F32(ROPE_THETA), -exponents)
    steps = jnp.concatenate([jnp.arange(128) * 128, jnp.arange(8) * 16 + s]).astype(F32)
    angles = steps[:, None] * jnp.concatenate([inverse, inverse])[None, :]
    cosine, sine = jnp.cos(angles), jnp.sin(angles)
    queries, own = front(
        [frame_slot[None], patch_count[None], vis_start[None]],
        [
            vit_states,
            vit_qkv_w,
            vit_out_w,
            text,
            vit_ln_gain[None],
            vit_ln_bias[None],
            vit_qkv_b[None],
            vit_out_b[None],
            pbias,
            attn_gain[None],
            cosine[:128],
            sine[:128],
            cosine[128:],
            sine[128:],
            proj_b[None],
        ],
        [proj_w, wq, wk, wv],
    )
    ctx, wo_all = attention(queries, own, wo)
    ctx = ctx.transpose(1, 2, 4, 0, 3, 5).reshape(256, 1024)
    partial = jnp.dot(ctx, wo_all.reshape(1024, 4096), preferred_element_type=F32)
    keep = jnp.where(core == 0, partial[:128], partial[128:])
    give = jnp.where(core == 0, partial[128:], partial[:128]).astype(BF)
    mixed = (keep + swap_cores(give).astype(F32)).astype(BF)
    return mixed.reshape(128, 1, 4096)


def solution(mesh):
    return jax.shard_map(
        per_device,
        mesh=mesh,
        in_specs=(
            P(("frame", "seq"), None, None),
            P(),
            P(),
            P(),
            P(None, ("frame", "seq"), None),
            P(),
            P(),
            P("seq", None),
            P(),
            P("seq", None),
            P(),
            P(),
            P(),
            P(),
            P(None, "frame"),
            P(None, "frame"),
            P(None, "frame"),
            P("frame", None),
        ),
        out_specs=P(None, ("frame", "seq"), None),
        check_vma=False,
    )
```

```python
import functools
import math

import jax
import jax.numpy as jnp
from jax import lax
from jax.experimental import pallas as pl
from jax.experimental.pallas import tpu as pltpu
from jax.sharding import PartitionSpec as P

MESH = pl.DeviceIdType.MESH
BF = jnp.bfloat16
F32 = jnp.float32
NEG = -1e30
ROPE_THETA = 500000.0
NEAR_FIRST = (1, 3, 2)


def remote(src, dst, send, recv, f, s):
    return pltpu.make_async_remote_copy(
        src_ref=src,
        dst_ref=dst,
        send_sem=send,
        recv_sem=recv,
        device_id={"frame": f, "seq": s},
        device_id_type=MESH,
    )


def places():
    f = lax.axis_index("frame")
    s = lax.axis_index("seq")
    y, z = s // 4, s % 4

    def along_y(k):
        return (y + k) % 4 * 4 + z

    def along_z(k):
        return y * 4 + (z + k) % 4

    def along_x(k):
        return (f // 2 + k) % 4 * 2 + f % 2

    partner = f + 1 - 2 * (f % 2)
    return f, s, along_x, along_y, along_z, partner


def greet(peers):
    barrier = pltpu.get_barrier_semaphore()
    for f, s in peers:
        pl.semaphore_signal(
            barrier, inc=1, device_id={"frame": f, "seq": s}, device_id_type=MESH
        )
    pl.semaphore_wait(barrier, len(peers))


def turned(row, eye):
    return jnp.sum(jnp.where(eye, row.astype(F32), 0.0), axis=1, keepdims=True).astype(jnp.int32)


def front_kernel(
    slot_r, count_r, start_r, v, qkvw, outw, t, vec, trig,
    proj, wq, wk, wv, wo,
    q_out, kv_out, wo_half,
    ws, wg, vp, tg, pw, wc, fold, plain, st, nrm, qk, vv, ctx, ctxo, pool, poolo, tok, land, table, col,
    local, wss, wrs, tss, trs, hss, hrs, vss, vrs, ess, ers, sss, srs, xss, xrs, pss, prs, oss, ors,
):
    f, s, xs, ys, zs, fp = places()
    core = f % 2

    def seq_at(k):
        return (s + k) % 16

    def lanes(first):
        return pl.ds(pl.multiple_of(first + core * 640, 128), 640)

    def landed(dst, recv):
        remote(dst, dst, vss, recv, fp, s).wait_recv()

    ln_g, ln_b = vec[:, :1280], vec[:, 1280:2560]
    pb, again = vec[:, 7680:11776], vec[:, 11776:]
    packs = [
        pltpu.make_async_copy(qkvw.at[:, lanes(0)], ws.at[0, :, pl.ds(0, 640)], local.at[0]),
        pltpu.make_async_copy(qkvw.at[:, lanes(1280)], ws.at[0, :, pl.ds(640, 640)], local.at[1]),
        pltpu.make_async_copy(qkvw.at[:, lanes(2560)], ws.at[1, :, pl.ds(0, 640)], local.at[2]),
        pltpu.make_async_copy(outw.at[:, lanes(0)], ws.at[1, :, pl.ds(640, 640)], local.at[3]),
    ]
    loads = [
        pltpu.make_async_copy(wq, wc.at[:, pl.ds(0, 256)], local.at[4]),
        pltpu.make_async_copy(wk, wc.at[:, pl.ds(256, 128)], local.at[5]),
        pltpu.make_async_copy(wv, wc.at[:, pl.ds(384, 128)], local.at[6]),
        pltpu.make_async_copy(proj, pw, local.at[7]),
    ]
    for copy in packs:
        copy.start()
    greet(
        [(f, seq_at(k)) for k in range(1, 16)]
        + [(xs(k), s) for k in (1, 2, 3)]
        + [(fp, s)]
    )
    for copy in packs:
        copy.wait()
    sends = []

    def go(copy):
        copy.start()
        sends.append(copy)

    def weight_slot(h, j, k):
        a, b = (4 - j) % 4, (4 - k) % 4
        if h == 0:
            return wg.at[0, ys(a) // 4 * 4 + zs(b) % 4]
        return wg.at[1, ys(b) // 4 * 4 + zs(a) % 4]

    def weight_half(ref, n):
        return ref.at[:, pl.ds(n * 640, 640)]

    def send_weights(j, k):
        for h in range(2):
            first, second = (ys, zs) if h == 0 else (zs, ys)
            slot = weight_slot(h, j, k)
            full = ws.at[h] if j == k == 0 else slot
            plan = []
            if j == k == 0:
                plan += [(full, slot, (1, 0, 0), first(1)), (full, slot, (3, 0, 0), first(3))]
            if k == 0 and j in (1, 3):
                part = weight_half(slot, j // 2)
                plan += [(part, part, (2, 0, j // 2), first(j))]
            if k == 0:
                plan += [(full, slot, (j, 1, 0), second(1)), (full, slot, (j, 3, 0), second(3))]
            if k in (1, 3):
                part = weight_half(slot, k // 2)
                plan += [(part, part, (j, 2, k // 2), second(k))]
            for n, (a, b, (jj, kk, m), to) in enumerate(plan):
                go(remote(a, b, wss.at[h, j, k, n], wrs.at[h, jj, kk, m], f, to))

    def take_weights(j, k):
        for h in range(2):
            slot = weight_slot(h, j, k)
            if k == 2 or (j == 2 and k == 0):
                landed(weight_half(slot, 0), wrs.at[h, j, k, 0])
                landed(weight_half(slot, 1), wrs.at[h, j, k, 1])
            else:
                landed(slot, wrs.at[h, j, k, 0])
        send_weights(j, k)

    send_weights(0, 0)
    go(remote(v, vp, vss, vrs, fp, s))
    go(remote(t, tg.at[f], tss.at[0], trs.at[1], xs(1), s))
    go(remote(t, tg.at[f], tss.at[1], trs.at[3], xs(3), s))
    go(remote(t, tg.at[f], hss.at[0, 0], hrs.at[0, 0], fp, s))
    for copy in loads:
        copy.start()
    wg[0, s] = ws[0]
    wg[1, s] = ws[1]
    slot = slot_r[...]
    holder = slot // 2
    pair = holder // 32 * 16 + holder % 16
    order = holder // 16 % 2 * 2 + slot % 2
    eye = lax.broadcasted_iota(jnp.int32, (128, 128), 0) == lax.broadcasted_iota(
        jnp.int32, (128, 128), 1
    )
    pair_c, order_c = turned(pair, eye), turned(order, eye)
    same = pair_c == pair
    rank = jnp.sum(jnp.where(same & (order_c < order), 1.0, 0.0), axis=0, keepdims=True).astype(
        jnp.int32
    )
    col[:, 0:1] = pair_c * 8 + turned(rank, eye) * 4
    col[:, 1:2] = turned(start_r[...], eye)
    col[:, 2:3] = turned(count_r[...], eye)
    facts = []
    for a in range(2):
        mine = (pair == f // 2 * 16 + s) & (rank == a)
        facts.append(
            [
                jnp.sum(
                    jnp.where(mine, row.astype(F32), 0.0), axis=1, keepdims=True
                ).astype(jnp.int32)
                for row in (order, count_r[...], start_r[...])
            ]
        )
    for copy in loads:
        copy.wait()

    def fold_rows(i, carry):
        rows = pl.ds(pl.multiple_of(i * 128, 128), 128)
        to = pl.ds(pl.multiple_of(i * 128 + i // 5 * 128, 128), 128)
        gained = (pw[rows, :].astype(F32) * again).astype(BF)
        fold[to, :] = jnp.dot(gained, wc[...], preferred_element_type=F32).astype(BF)
        return carry

    def text_rows(source, at):
        plain[:, at] = jnp.dot(source[...], wc[...], preferred_element_type=F32).reshape(4, 32, 512)

    def text_half(ref, n):
        return ref.at[pl.ds(n * 64, 64)]

    lax.fori_loop(0, 3, fold_rows, 0)
    take_weights(1, 0)
    take_weights(3, 0)
    lax.fori_loop(3, 6, fold_rows, 0)
    take_weights(0, 1)
    take_weights(0, 3)
    take_weights(2, 0)
    lax.fori_loop(6, 8, fold_rows, 0)
    take_weights(1, 1)
    take_weights(1, 3)
    lax.fori_loop(8, 10, fold_rows, 0)
    take_weights(3, 1)
    take_weights(3, 3)
    row = lax.broadcasted_iota(jnp.int32, (16, 1), 0)
    biased = pb * again
    upper = biased.astype(BF).astype(F32)
    biased = jnp.where(row == 0, upper, jnp.where(row == 1, biased - upper, 0.0)).astype(BF)
    biased = jnp.dot(biased, wc[...], preferred_element_type=F32)
    biased = jnp.sum(biased, axis=0, keepdims=True)
    first = lax.broadcasted_iota(jnp.int32, (128, 512), 0) == 0
    fold[640:768, :] = jnp.where(first, biased, 0.0).astype(BF)
    fold[1408:1536, :] = jnp.zeros((128, 512), BF)
    text_rows(t, f)
    landed(vp, vrs)
    for a in range(2):
        pick = facts[a][0]
        chosen = jnp.zeros((256, 1280), F32)
        for n in range(2):
            chosen = jnp.where(pick == core * 2 + n, v[n].astype(F32), chosen)
            chosen = jnp.where(pick == 2 - core * 2 + n, vp[n].astype(F32), chosen)
        st[a * 256 : a * 256 + 256, :] = chosen.astype(BF)

    def norm_rows(i, carry):
        rows = pl.ds(pl.multiple_of(i * 128, 128), 128)
        x = st[rows, :].astype(F32)
        centred = x - jnp.mean(x, axis=1, keepdims=True)
        spread = jnp.mean(centred * centred, axis=1, keepdims=True)
        nrm[rows, :] = (centred * lax.rsqrt(spread + 1e-6) * ln_g + ln_b).astype(BF)
        return carry

    lax.fori_loop(0, 4, norm_rows, 0)
    take_weights(2, 1)
    take_weights(2, 3)
    for j in (1, 3):
        fs = xs(4 - j)
        here = tg.at[fs]
        landed(here, trs.at[j])
        part = text_half(here, j // 2)
        go(remote(part, part, tss.at[2 + j // 2], hrs.at[2, j // 2], xs(j), s))
        go(remote(here, here, hss.at[1, j // 2], hrs.at[1, j // 2], fp, s))
    for n in range(2):
        half = pl.ds(n * 128, 128)
        go(remote(wo.at[half], wo_half.at[n], oss.at[n], ors.at[n], xs(1 + 2 * n), s))
    for j in (1, 3):
        text_rows(tg.at[xs(4 - j)], xs(4 - j))
    landed(tg.at[fp], hrs.at[0, 0])
    text_rows(tg.at[fp], fp)
    take_weights(0, 2)
    for j in (1, 3):
        fs = xs(4 - j) + 1 - 2 * core
        landed(tg.at[fs], hrs.at[1, j // 2])
        text_rows(tg.at[fs], fs)
    take_weights(1, 2)
    take_weights(3, 2)
    far = xs(2)
    for n in range(2):
        part = text_half(tg.at[far], n)
        landed(part, hrs.at[2, n])
        go(remote(part, part, hss.at[2, n], hrs.at[3, n], fp, s))
    text_rows(tg.at[far], far)
    far = far + 1 - 2 * core
    for n in range(2):
        landed(text_half(tg.at[far], n), hrs.at[3, n])
    text_rows(tg.at[far], far)
    take_weights(2, 2)

    def project(i, carry):
        rows = pl.ds(pl.multiple_of(i * 128, 128), 128)
        n = nrm[rows, :]
        both = jnp.dot(n, wg[0].reshape(1280, 1280), preferred_element_type=F32)
        qk[rows, :640] = (both[:, :640] + vec[:, lanes(3840)]).astype(BF)
        qk[rows, 640:] = (both[:, 640:] + vec[:, lanes(5120)]).astype(BF)
        third = jnp.dot(n, wg[1, :, :, :640].reshape(1280, 640), preferred_element_type=F32)
        vv[rows, :] = (third + vec[:, lanes(6400)]).astype(BF)
        return carry

    lax.fori_loop(0, 4, project, 0)
    for a in range(2):
        live = lax.broadcasted_iota(jnp.int32, (1, 256), 1) < facts[a][1]
        rows = slice(a * 256, a * 256 + 256)
        for h in range(8):
            q = qk[rows, h * 80 : h * 80 + 80]
            k = qk[rows, 640 + h * 80 : 640 + h * 80 + 80]
            val = vv[rows, h * 80 : h * 80 + 80]
            scores = lax.dot_general(
                q, k, (((1,), (1,)), ((), ())), preferred_element_type=F32
            ) * (1.0 / math.sqrt(80))
            scores = jnp.where(live, scores, NEG)
            weights = jnp.exp(scores - jnp.max(scores, axis=1, keepdims=True))
            prob = (weights / jnp.sum(weights, axis=1, keepdims=True)).astype(BF)
            ctx[rows, h * 80 : h * 80 + 80] = jnp.dot(
                prob, val, preferred_element_type=F32
            ).astype(BF)
    go(remote(ctx, ctxo, ess.at[0], ers.at[0], fp, s))

    def out_rows(owner):
        return wg[1, pl.ds(owner * 8, 8), :, 640:].reshape(640, 640)

    attended = jnp.dot(ctx[...], out_rows(core), preferred_element_type=F32)
    landed(ctxo, ers.at[0])
    attended = attended + jnp.dot(ctxo[...], out_rows(1 - core), preferred_element_type=F32)
    hidden = (st[:, lanes(0)].astype(F32) + attended + vec[:, lanes(2560)]).astype(BF)
    quarter = lax.broadcasted_iota(jnp.int32, (128, 512), 1) // 4 == lax.broadcasted_iota(
        jnp.int32, (128, 512), 0
    )
    pooled = jnp.dot(
        jnp.where(quarter, 0.25, 0.0).astype(BF), hidden, preferred_element_type=F32
    )
    pool[...] = pooled.astype(BF)
    go(remote(pool, poolo, ess.at[1], ers.at[1], fp, s))
    landed(poolo, ers.at[1])

    def square(c, total):
        cols = pl.ds(pl.multiple_of(c * 512, 128), 512)
        own_rows = pl.ds(pl.multiple_of(core * 640, 128), 640)
        other_rows = pl.ds(pl.multiple_of(640 - core * 640, 128), 640)
        seen = jnp.dot(pool[...], pw[own_rows, cols], preferred_element_type=F32)
        seen = seen + jnp.dot(poolo[...], pw[other_rows, cols], preferred_element_type=F32)
        seen = seen + vec[:, pl.ds(pl.multiple_of(7680 + c * 512, 128), 512)]
        return total + jnp.sum(seen * seen, axis=1, keepdims=True)

    total = lax.fori_loop(0, 8, square, jnp.zeros((128, 1), F32))
    scale = lax.rsqrt(total * (1.0 / 4096) + 1e-5)
    head = (pool[...].astype(F32) * scale).astype(BF)
    tail = jnp.where(lax.broadcasted_iota(jnp.int32, (128, 128), 1) == 0, scale, 0.0).astype(BF)
    want = lax.broadcasted_iota(jnp.int32, (128, 1), 0)
    frame_of = want // 4 % 2
    begin = jnp.where(frame_of == 0, facts[0][2], facts[1][2])
    token = (want // 8 - begin + 16384) % 16 + want % 4 * 16 + frame_of * 64
    taken = (token == lax.broadcasted_iota(jnp.int32, (128, 128), 1)).astype(F32).astype(BF)
    head = jnp.dot(taken, head, preferred_element_type=F32)
    tail = jnp.dot(taken, tail, preferred_element_type=F32)
    for i in range(16):
        tok[i, :, :640] = head[i * 8 : i * 8 + 8].astype(BF)
        tok[i, :, 640:] = tail[i * 8 : i * 8 + 8].astype(BF)
    for k in range(1, 16):
        go(remote(tok.at[seq_at(k)], land.at[s], sss.at[k], srs.at[k], f, seq_at(k)))
    land[s] = tok[s]
    for k in range(1, 16):
        landed(land.at[seq_at(16 - k)], srs.at[k])
    for i, k in enumerate(NEAR_FIRST):
        go(remote(land, table.at[f], xss.at[i], xrs.at[k], xs(k), s))
    go(remote(land, table.at[f], pss.at[0], prs.at[0], fp, s))
    table[f] = land[...]
    for j in NEAR_FIRST:
        fs = xs(4 - j)
        landed(table.at[fs], xrs.at[j])
        go(remote(table.at[fs], table.at[fs], pss.at[j], prs.at[j], fp, s))
    for j in range(4):
        landed(table.at[(f // 2 + 4 - j) % 4 * 2 + 1 - core], prs.at[j])
    parts = []
    for x in range(4):
        even = table[2 * x].astype(F32).reshape(128, 768).astype(BF)
        odd = table[2 * x + 1].astype(F32).reshape(128, 768).astype(BF)
        part = jnp.dot(even, fold[:768, :], preferred_element_type=F32)
        part = part + jnp.dot(odd, fold[768:, :], preferred_element_type=F32)
        parts.append(part.astype(BF))
    visual = jnp.concatenate(parts, axis=0)
    sign = jnp.where(lax.broadcasted_iota(jnp.int32, (1, 128), 1) < 64, -1.0, 1.0)
    factor = math.log2(math.e) / math.sqrt(128)
    for blk in range(4):
        some = slice(blk * 32, blk * 32 + 32)
        shape = (8, 32, 1)
        frame = lax.broadcasted_iota(jnp.int32, shape, 1) + blk * 32
        owner = lax.broadcasted_iota(jnp.int32, shape, 0)
        within = frame * 128 + owner * 16 + s - col[some, 1:2][None]
        live = (within >= 0) & (within < col[some, 2:3][None] // 4)
        source = jnp.where(live, col[some, 0:1][None] + within // 16, -1).reshape(256, 1)
        chosen = (source == lax.broadcasted_iota(jnp.int32, (256, 512), 1)).astype(F32).astype(BF)
        placed = jnp.dot(chosen, visual, preferred_element_type=F32)
        x = jnp.where(source >= 0, placed, plain[blk].reshape(256, 512))
        c1, s1 = trig[0, some, :][None], trig[1, some, :][None]
        c2, s2 = trig[0, 128:, :][:, None, :], trig[1, 128:, :][:, None, :]
        cosine = (c1 * c2 - s1 * s2).reshape(256, 128)
        sine = (s1 * c2 + c1 * s2).reshape(256, 128) * sign

        def rotate(n):
            part = x[:, n * 128 : n * 128 + 128]
            return part * cosine + pltpu.roll(part, 64, 1) * sine

        for h in range(2):
            q_out[blk, h * 256 : h * 256 + 256, :] = (rotate(h) * factor).astype(BF)
        rows = slice(blk % 2 * 256, blk % 2 * 256 + 256)
        kv_out[blk // 2, rows, :128] = rotate(2).astype(BF)
        kv_out[blk // 2, rows, 128:] = x[:, 384:].astype(BF)
    for n in range(2):
        landed(wo_half.at[n], ors.at[n])
    for copy in sends:
        copy.wait_send()


def front(rows, vmem_args, hbm_args):
    shape = jax.ShapeDtypeStruct
    dma = pltpu.SemaphoreType.DMA
    vmem = pl.BlockSpec(memory_space=pltpu.VMEM)
    hbm = pl.BlockSpec(memory_space=pl.ANY)
    buf = pltpu.VMEM
    return pl.pallas_call(
        front_kernel,
        out_shape=(
            shape((4, 512, 128), BF),
            shape((2, 512, 256), BF),
            shape((2, 128, 4096), BF),
        ),
        in_specs=[vmem] * (len(rows) + len(vmem_args)) + [hbm] * len(hbm_args),
        out_specs=(vmem, vmem, hbm),
        scratch_shapes=[
            buf((2, 80, 1280), BF),
            buf((2, 16, 80, 1280), BF),
            buf((2, 256, 1280), BF),
            buf((8, 128, 4096), BF),
            buf((1280, 4096), BF),
            buf((4096, 512), BF),
            buf((1536, 512), BF),
            buf((4, 8, 32, 512), F32),
            buf((512, 1280), BF),
            buf((512, 1280), BF),
            buf((512, 1280), BF),
            buf((512, 640), BF),
            buf((512, 640), BF),
            buf((512, 640), BF),
            buf((128, 640), BF),
            buf((128, 640), BF),
            buf((16, 8, 768), BF),
            buf((16, 8, 768), BF),
            buf((8, 16, 8, 768), BF),
            buf((128, 128), jnp.int32),
            dma((8,)),
            dma((2, 4, 4, 4)),
            dma((2, 4, 4, 2)),
            dma((4,)),
            dma((4,)),
            dma((3, 2)),
            dma((4, 2)),
            dma,
            dma,
            dma((2,)),
            dma((2,)),
            dma((16,)),
            dma((16,)),
            dma((3,)),
            dma((4,)),
            dma((4,)),
            dma((4,)),
            dma((2,)),
            dma((2,)),
        ],
        compiler_params=pltpu.CompilerParams(
            collective_id=1, has_side_effects=True, vmem_limit_bytes=56 << 20
        ),
        name="front",
    )(*rows, *vmem_args, *hbm_args)


def attend(q_ref, acc, top, den, kv, tile, keys, base, inc):
    scores = lax.dot_general(
        q_ref[tile], kv[:keys, :128], (((1,), (1,)), ((), ())), preferred_element_type=F32
    )
    if base is not None:
        row = lax.broadcasted_iota(jnp.int32, (512, 1), 0) % 256
        col = lax.broadcasted_iota(jnp.int32, (1, keys), 1)
        row = row % 32 * 8 + row // 32 + base + inc
        col = col // 256 * 256 + col % 32 * 8 + col % 256 // 32
        scores = jnp.where(col < row, scores, NEG)
    old = top[tile]
    new = jnp.maximum(old, jnp.max(scores, axis=1, keepdims=True))
    fade = jnp.exp2(old - new)
    weights = jnp.exp2(scores - new[:, :1]).astype(BF)
    top[tile] = new
    wide = jnp.concatenate([kv[:keys, 128:], jnp.ones((keys, 128), BF)], axis=1)
    added = jnp.dot(weights, wide, preferred_element_type=F32)
    den[tile] = den[tile] * fade + added[:, 128:]
    acc[tile] = acc[tile] * fade + added[:, :128]


ORDER = (
    (0, 0), (1, 0), (3, 0), (0, 1), (0, 3), (2, 0), (1, 1), (1, 3),
    (3, 1), (3, 3), (0, 2), (2, 1), (2, 3), (1, 2), (3, 2), (2, 2),
)


def attention_kernel(
    q, own, wo, wo_half, out, kv, acc, top, den, ctx, seen, lhs, wog, give, got,
    local, ss, rs, css, crs, oss, ors, gss, grs,
):
    f, s, xs, ys, zs, fp = places()
    core = f % 2
    y, z = s // 4, s % 4
    greet(
        [(f, ys(1)), (f, ys(3)), (f, zs(1)), (f, zs(3))]
        + [(xs(k), s) for k in (1, 2, 3)]
        + [(fp, s)]
    )

    def slot_of(h, j, k):
        a, b = (4 - j) % 4, (4 - k) % 4
        if h == 0:
            return kv.at[0, ys(a) // 4 * 4 + zs(b) % 4]
        return kv.at[1, ys(b) // 4 * 4 + zs(a) % 4]

    def half_of(ref, n):
        return ref.at[pl.ds(n * 256, 256)]

    def copies_of(j, k):
        result = []
        for h in range(2):
            first, second = (ys, zs) if h == 0 else (zs, ys)
            slot = slot_of(h, j, k)
            full = own.at[h] if j == k == 0 else slot
            plan = []
            if j == k == 0:
                plan += [(full, slot, (1, 0, 0), first(1)), (full, slot, (3, 0, 0), first(3))]
            if k == 0 and j in (1, 3):
                part = half_of(slot, j // 2)
                plan += [(part, part, (2, 0, j // 2), first(j))]
            if k == 0:
                plan += [(full, slot, (j, 1, 0), second(1)), (full, slot, (j, 3, 0), second(3))]
            if k in (1, 3):
                part = half_of(slot, k // 2)
                plan += [(part, part, (j, 2, k // 2), second(k))]
            for n, (a, b, (jj, kk, m), to) in enumerate(plan):
                result.append(remote(a, b, ss.at[h, j, k, n], rs.at[h, jj, kk, m], f, to))
        return result

    def landed(dst, recv):
        remote(dst, dst, local.at[0], recv, fp, s).wait_recv()

    def take(j, k):
        for h in range(2):
            slot = slot_of(h, j, k)
            if k == 2 or (j == 2 and k == 0):
                landed(half_of(slot, 0), rs.at[h, j, k, 0])
                landed(half_of(slot, 1), rs.at[h, j, k, 1])
            else:
                landed(slot, rs.at[h, j, k, 0])

    for copy in copies_of(0, 0):
        copy.start()
    lower, upper = pl.ds(0, 128), pl.ds(128, 128)
    parts = [
        remote(wo_half.at[0], wog.at[2, lower], oss.at[0], ors.at[0], xs(1), s),
        remote(wo_half.at[1], wog.at[2, upper], oss.at[1], ors.at[1], xs(3), s),
        remote(wo.at[upper], wog.at[3, upper], oss.at[2], ors.at[2], xs(1), s),
        remote(wo.at[lower], wog.at[1, lower], oss.at[3], ors.at[3], xs(3), s),
    ]
    keeps = [
        pltpu.make_async_copy(wo, wog.at[0], local.at[1]),
        pltpu.make_async_copy(wo_half.at[0], wog.at[3, lower], local.at[2]),
        pltpu.make_async_copy(wo_half.at[1], wog.at[1, upper], local.at[3]),
    ]
    for copy in parts + keeps:
        copy.start()
    kv[0, s] = own[0]
    kv[1, s] = own[1]
    top[...] = jnp.full_like(top, NEG)
    den[...] = jnp.zeros_like(den)
    acc[...] = jnp.zeros_like(acc)

    def step(i, carry):
        j = k = 0
        for n, (jj, kk) in enumerate(ORDER):
            if n > 0:
                j = jnp.where(i == n, jj, j)
                k = jnp.where(i == n, kk, k)

                @pl.when(i == n)
                def _(jj=jj, kk=kk):
                    take(jj, kk)
                    for copy in copies_of(jj, kk):
                        copy.start()

        a = (y + 4 - j) % 4 * 4 + (z + 4 - k) % 4
        b = (y + 4 - k) % 4 * 4 + (z + 4 - j) % 4
        at = functools.partial(attend, q, acc, top, den)
        inc = jnp.where(a <= s, 1, 0)
        at(kv.at[0, a], 0, 256, 0, inc)
        at(kv.at[0, a], 1, 512, 256, inc)
        at(kv.at[0, a], 2, 512, None, inc)
        at(kv.at[0, a], 3, 512, None, inc)
        inc = jnp.where(b <= s, 1, 0)
        at(kv.at[1, b], 2, 256, 0, inc)
        at(kv.at[1, b], 3, 512, 256, inc)
        return carry

    lax.fori_loop(0, 16, step, 0)
    for tile in range(4):
        block = (acc[tile] / den[tile]).astype(BF)
        for head in range(2):
            for owner in range(8):
                start = head * 256 + owner * 32
                ctx[owner // 2, owner % 2, tile, head] = block[start : start + 32]
    for j, k in ORDER:
        for copy in copies_of(j, k):
            copy.wait_send()
    x = f // 2
    last = []
    for i, k in enumerate(NEAR_FIRST):
        last.append(remote(ctx.at[(x + k) % 4], seen.at[4 - k], css.at[i], crs.at[k], xs(k), s))
    for copy in last:
        copy.start()
    seen[0] = ctx[x]
    for copy in keeps:
        copy.wait()
    for copy in parts:
        copy.wait()
    for k in (1, 3, 2):
        landed(seen.at[4 - k], crs.at[k])
    for d in range(4):
        for head in range(2):
            cols = slice(d * 256 + head * 128, d * 256 + head * 128 + 128)
            for owner in range(2):
                lhs[owner, :, cols] = seen[d, owner, :, head].reshape(128, 128)

    def columns(c):
        return pl.ds(pl.multiple_of(c * 512, 128), 512)

    def share(c):
        return remote(
            give.at[:, columns(c)], got.at[:, columns(c)], gss.at[c], grs.at[c], fp, s
        )

    def partial(owner, c):
        return jnp.dot(
            lhs[owner], wog[:, :, columns(c)].reshape(1024, 512), preferred_element_type=F32
        )

    def to_partner(c, carry):
        give[:, columns(c)] = partial(1 - core, c).astype(BF)

        @pl.when(c > 0)
        def _():
            share(c - 1).start()

        return carry

    def to_output(c, carry):
        mine = partial(core, c)

        @pl.when(c == 0)
        def _():
            share(7).start()

        share(c).wait()
        out[:, columns(c)] = (mine + got[:, columns(c)].astype(F32)).astype(BF)
        return carry

    lax.fori_loop(0, 8, to_partner, 0)
    lax.fori_loop(0, 8, to_output, 0)
    for copy in last:
        copy.wait_send()


def attention(q, own, wo, wo_half):
    dma = pltpu.SemaphoreType.DMA
    vmem = pl.BlockSpec(memory_space=pltpu.VMEM)
    hbm = pl.BlockSpec(memory_space=pl.ANY)
    state = pltpu.VMEM((4, 512, 128), F32)
    return pl.pallas_call(
        attention_kernel,
        out_shape=jax.ShapeDtypeStruct((128, 4096), BF),
        in_specs=[vmem, vmem, hbm, hbm],
        out_specs=vmem,
        scratch_shapes=[
            pltpu.VMEM((2, 16, 512, 256), BF),
            state,
            state,
            state,
            pltpu.VMEM((4, 2, 4, 2, 32, 128), BF),
            pltpu.VMEM((4, 2, 4, 2, 32, 128), BF),
            pltpu.VMEM((2, 128, 1024), BF),
            pltpu.VMEM((4, 256, 4096), BF),
            pltpu.VMEM((128, 4096), BF),
            pltpu.VMEM((128, 4096), BF),
            dma((4,)),
            dma((2, 4, 4, 4)),
            dma((2, 4, 4, 2)),
            dma((3,)),
            dma((4,)),
            dma((4,)),
            dma((4,)),
            dma((8,)),
            dma((8,)),
        ],
        compiler_params=pltpu.CompilerParams(
            collective_id=3, has_side_effects=True, vmem_limit_bytes=48 << 20
        ),
        name="attention",
    )(q, own, wo, wo_half)


def per_device(
    vit_states,
    frame_slot,
    patch_count,
    vis_start,
    text_embed,
    vit_ln_gain,
    vit_ln_bias,
    vit_qkv_w,
    vit_qkv_b,
    vit_out_w,
    vit_out_b,
    proj_w,
    proj_b,
    attn_gain,
    wq,
    wk,
    wv,
    wo,
):
    s = lax.axis_index("seq")
    text = text_embed.reshape(128, 4096).astype(F32)
    text = (
        text * lax.rsqrt(jnp.mean(text * text, axis=1, keepdims=True) + 1e-5) * attn_gain
    ).astype(BF)
    exponents = jnp.arange(0, 128, 2).astype(F32) / 128
    inverse = jnp.power(F32(ROPE_THETA), -exponents)
    steps = jnp.concatenate([jnp.arange(128) * 128, jnp.arange(8) * 16 + s]).astype(F32)
    angles = steps[:, None] * jnp.concatenate([inverse, inverse])[None, :]
    trig = jnp.stack([jnp.cos(angles), jnp.sin(angles)])
    vectors = [vit_ln_gain, vit_ln_bias, vit_out_b, vit_qkv_b, proj_b, attn_gain]
    queries, own, wo_half = front(
        [frame_slot[None], patch_count[None], vis_start[None]],
        [vit_states, vit_qkv_w, vit_out_w, text, jnp.concatenate(vectors)[None], trig],
        [proj_w, wq, wk, wv, wo],
    )
    return attention(queries, own, wo, wo_half).reshape(128, 1, 4096)


def solution(mesh):
    return jax.shard_map(
        per_device,
        mesh=mesh,
        in_specs=(
            P(("frame", "seq"), None, None),
            P(),
            P(),
            P(),
            P(None, ("frame", "seq"), None),
            P(),
            P(),
            P("seq", None),
            P(),
            P("seq", None),
            P(),
            P(),
            P(),
            P(),
            P(None, "frame"),
            P(None, "frame"),
            P(None, "frame"),
            P("frame", None),
        ),
        out_specs=P(None, ("frame", "seq"), None),
        check_vma=False,
    )
```

```python
import functools
import math

import jax
import jax.numpy as jnp
from jax import lax
from jax.experimental import pallas as pl
from jax.experimental.pallas import tpu as pltpu
from jax.sharding import PartitionSpec as P

MESH = pl.DeviceIdType.MESH
BF = jnp.bfloat16
F32 = jnp.float32
NEG = -1e30
ROPE_THETA = 500000.0
NEAR_FIRST = (1, 3, 2)


def remote(src, dst, send, recv, f, s):
    return pltpu.make_async_remote_copy(
        src_ref=src,
        dst_ref=dst,
        send_sem=send,
        recv_sem=recv,
        device_id={"frame": f, "seq": s},
        device_id_type=MESH,
    )


def places():
    f = lax.axis_index("frame")
    s = lax.axis_index("seq")
    y, z = s // 4, s % 4

    def along_y(k):
        return (y + k) % 4 * 4 + z

    def along_z(k):
        return y * 4 + (z + k) % 4

    def along_x(k):
        return (f // 2 + k) % 4 * 2 + f % 2

    partner = f + 1 - 2 * (f % 2)
    return f, s, along_x, along_y, along_z, partner


def greet(peers):
    barrier = pltpu.get_barrier_semaphore()
    for f, s in peers:
        pl.semaphore_signal(
            barrier, inc=1, device_id={"frame": f, "seq": s}, device_id_type=MESH
        )
    pl.semaphore_wait(barrier, len(peers))


def turned(row, eye):
    return jnp.sum(jnp.where(eye, row.astype(F32), 0.0), axis=1, keepdims=True).astype(jnp.int32)


def front_kernel(
    slot_r, count_r, start_r, v, qkvw, outw, t_raw, ln_gr, ln_br, outb, qkvb, pbr, gainr, trig,
    proj, wq, wk, wv, wo,
    q_out, kv_out, wo_half,
    t, ws, wg, vp, tg, pw, wc, fold, plain, st, nrm, qk, vv, ctx, ctxo, pool, poolo, tok, land, table, col, prow,
    local, wss, wrs, tss, trs, hss, hrs, vss, vrs, ess, ers, sss, srs, xss, xrs, pss, prs, oss, ors, fxr, fps, fpr,
):
    f, s, xs, ys, zs, fp = places()
    core = f % 2

    def seq_at(k):
        return (s + k) % 16

    def lanes(first):
        return pl.ds(pl.multiple_of(first + core * 640, 128), 640)

    def halved(ref, first):
        row = ref[...][None]
        return jnp.where(
            core == 0, row[:, first : first + 640], row[:, first + 640 : first + 1280]
        )

    def landed(dst, recv):
        remote(dst, dst, vss, recv, fp, s).wait_recv()

    ln_g, ln_b = ln_gr[...][None], ln_br[...][None]
    pb, again = pbr[...][None], gainr[...][None]
    packs = [
        pltpu.make_async_copy(qkvw.at[:, lanes(0)], ws.at[0, :, pl.ds(0, 640)], local.at[0]),
        pltpu.make_async_copy(qkvw.at[:, lanes(1280)], ws.at[0, :, pl.ds(640, 640)], local.at[1]),
        pltpu.make_async_copy(qkvw.at[:, lanes(2560)], ws.at[1, :, pl.ds(0, 640)], local.at[2]),
        pltpu.make_async_copy(outw.at[:, lanes(0)], ws.at[1, :, pl.ds(640, 640)], local.at[3]),
    ]
    loads = [
        pltpu.make_async_copy(wq, wc.at[:, pl.ds(0, 256)], local.at[4]),
        pltpu.make_async_copy(wk, wc.at[:, pl.ds(256, 128)], local.at[5]),
        pltpu.make_async_copy(wv, wc.at[:, pl.ds(384, 128)], local.at[6]),
        pltpu.make_async_copy(proj, pw, local.at[7]),
    ]
    for copy in packs + loads:
        copy.start()
    for i in range(4):
        rows = slice(i * 32, i * 32 + 32)
        x = t_raw[rows, :].astype(F32)
        x = x * lax.rsqrt(jnp.mean(x * x, axis=1, keepdims=True) + 1e-5)
        t[rows, :] = (x * again).astype(BF)
    greet(
        [(f, seq_at(k)) for k in range(1, 16)]
        + [(xs(k), s) for k in (1, 2, 3)]
        + [(fp, s)]
    )
    for copy in packs:
        copy.wait()
    sends = []

    def go(copy):
        copy.start()
        sends.append(copy)

    def weight_slot(h, j, k):
        a, b = (4 - j) % 4, (4 - k) % 4
        if h == 0:
            return wg.at[0, ys(a) // 4 * 4 + zs(b) % 4]
        return wg.at[1, ys(b) // 4 * 4 + zs(a) % 4]

    def weight_half(ref, n):
        return ref.at[:, pl.ds(n * 640, 640)]

    def weight_copy(h, j, k, n, a, b, at, to):
        go(remote(a, b, wss.at[h, j, k, n], wrs.at[(h,) + at], f, to))

    def start_weights():
        for h in range(2):
            first = (ys, zs)[h]
            slot = weight_slot(h, 0, 0)
            weight_copy(h, 0, 0, 0, ws.at[h], slot, (1, 0, 0), first(1))
            weight_copy(h, 0, 0, 1, ws.at[h], slot, (3, 0, 0), first(3))

    def pass_weights(j):
        for h in range(2):
            second = (zs, ys)[h]
            slot = weight_slot(h, j, 0)
            full = ws.at[h] if j == 0 else slot
            weight_copy(h, j, 0, 2, full, slot, (j, 1, 0), second(1))
            weight_copy(h, j, 0, 3, full, slot, (j, 3, 0), second(3))

    def relay_weights(j, k):
        for h in range(2):
            first, second = (ys, zs) if h == 0 else (zs, ys)
            n, at, to = (j // 2, (2, 0), first(j)) if k == 0 else (k // 2, (j, 2), second(k))
            part = weight_half(weight_slot(h, j, k), n)
            weight_copy(h, j, k, 0, part, part, at + (n,), to)

    def take_weights(j, k):
        for h in range(2):
            slot = weight_slot(h, j, k)
            if k == 2 or (j == 2 and k == 0):
                landed(weight_half(slot, 0), wrs.at[h, j, k, 0])
                landed(weight_half(slot, 1), wrs.at[h, j, k, 1])
            else:
                landed(slot, wrs.at[h, j, k, 0])
        if k in (1, 3):
            relay_weights(j, k)

    start_weights()
    go(remote(v, vp, vss, vrs, fp, s))
    go(remote(t, tg.at[f], tss.at[0], trs.at[1], xs(1), s))
    go(remote(t, tg.at[f], tss.at[1], trs.at[3], xs(3), s))
    go(remote(t, tg.at[f], hss.at[0, 0], hrs.at[0, 0], fp, s))
    wg[0, s] = ws[0]
    wg[1, s] = ws[1]
    slot = slot_r[...]
    holder = slot // 2
    pair = holder // 32 * 16 + holder % 16
    order = holder // 16 % 2 * 2 + slot % 2
    eye = lax.broadcasted_iota(jnp.int32, (128, 128), 0) == lax.broadcasted_iota(
        jnp.int32, (128, 128), 1
    )
    pair_c, order_c = turned(pair, eye), turned(order, eye)
    same = pair_c == pair
    rank = jnp.sum(jnp.where(same & (order_c < order), 1.0, 0.0), axis=0, keepdims=True).astype(
        jnp.int32
    )
    col[:, 0:1] = pair_c * 8 + turned(rank, eye) * 4
    col[:, 1:2] = turned(start_r[...], eye)
    col[:, 2:3] = turned(count_r[...], eye)
    facts = []
    for a in range(2):
        mine = (pair == f // 2 * 16 + s) & (rank == a)
        facts.append(
            [
                jnp.sum(
                    jnp.where(mine, row.astype(F32), 0.0), axis=1, keepdims=True
                ).astype(jnp.int32)
                for row in (order, count_r[...], start_r[...])
            ]
        )
    for copy in loads:
        copy.wait()

    def fold_rows(i, carry):
        rows = pl.ds(pl.multiple_of(i * 128, 128), 128)
        to = pl.ds(pl.multiple_of(i * 128 + i // 5 * 128, 128), 128)
        gained = (pw[rows, :].astype(F32) * again).astype(BF)
        fold[to, :] = jnp.dot(gained, wc[...], preferred_element_type=F32).astype(BF)
        return carry

    def text_rows(source, at):
        plain[:, at] = jnp.dot(source[...], wc[...], preferred_element_type=F32).reshape(4, 32, 512)

    def text_half(ref, n):
        return ref.at[pl.ds(n * 64, 64)]

    lax.fori_loop(0, 3, fold_rows, 0)
    take_weights(1, 0)
    take_weights(3, 0)
    relay_weights(1, 0)
    relay_weights(3, 0)
    pass_weights(0)
    lax.fori_loop(3, 6, fold_rows, 0)
    pass_weights(1)
    lax.fori_loop(6, 8, fold_rows, 0)
    take_weights(2, 0)
    pass_weights(2)
    pass_weights(3)
    take_weights(0, 1)
    take_weights(0, 3)
    lax.fori_loop(8, 10, fold_rows, 0)
    row = lax.broadcasted_iota(jnp.int32, (16, 1), 0)
    biased = pb * again
    upper = biased.astype(BF).astype(F32)
    biased = jnp.where(row == 0, upper, jnp.where(row == 1, biased - upper, 0.0)).astype(BF)
    biased = jnp.dot(biased, wc[...], preferred_element_type=F32)
    biased = jnp.sum(biased, axis=0, keepdims=True)
    first = lax.broadcasted_iota(jnp.int32, (128, 512), 0) == 0
    fold[640:768, :] = jnp.where(first, biased, 0.0).astype(BF)
    fold[1408:1536, :] = jnp.zeros((128, 512), BF)
    text_rows(t, f)
    take_weights(1, 1)
    take_weights(1, 3)
    landed(vp, vrs)
    for a in range(2):
        pick = facts[a][0]
        chosen = jnp.zeros((256, 1280), F32)
        for n in range(2):
            chosen = jnp.where(pick == core * 2 + n, v[n].astype(F32), chosen)
            chosen = jnp.where(pick == 2 - core * 2 + n, vp[n].astype(F32), chosen)
        st[a * 256 : a * 256 + 256, :] = chosen.astype(BF)

    def norm_rows(i, carry):
        rows = pl.ds(pl.multiple_of(i * 128, 128), 128)
        x = st[rows, :].astype(F32)
        centred = x - jnp.mean(x, axis=1, keepdims=True)
        spread = jnp.mean(centred * centred, axis=1, keepdims=True)
        nrm[rows, :] = (centred * lax.rsqrt(spread + 1e-6) * ln_g + ln_b).astype(BF)
        return carry

    lax.fori_loop(0, 4, norm_rows, 0)
    for j in (1, 3):
        fs = xs(4 - j)
        here = tg.at[fs]
        landed(here, trs.at[j])
        part = text_half(here, j // 2)
        go(remote(part, part, tss.at[2 + j // 2], hrs.at[2, j // 2], xs(j), s))
        go(remote(here, here, hss.at[1, j // 2], hrs.at[1, j // 2], fp, s))
    for n in range(2):
        half = pl.ds(n * 128, 128)
        go(remote(wo.at[half], wo_half.at[n], oss.at[n], ors.at[n], xs(1 + 2 * n), s))
    take_weights(2, 1)
    take_weights(2, 3)
    text_rows(tg.at[xs(3)], xs(3))
    take_weights(3, 1)
    take_weights(3, 3)
    text_rows(tg.at[xs(1)], xs(1))
    landed(tg.at[fp], hrs.at[0, 0])
    text_rows(tg.at[fp], fp)
    take_weights(0, 2)
    for j in (1, 3):
        fs = xs(4 - j) + 1 - 2 * core
        landed(tg.at[fs], hrs.at[1, j // 2])
        text_rows(tg.at[fs], fs)
    take_weights(1, 2)
    take_weights(3, 2)
    far = xs(2)
    for n in range(2):
        part = text_half(tg.at[far], n)
        landed(part, hrs.at[2, n])
        go(remote(part, part, hss.at[2, n], hrs.at[3, n], fp, s))
    text_rows(tg.at[far], far)
    far = far + 1 - 2 * core
    for n in range(2):
        landed(text_half(tg.at[far], n), hrs.at[3, n])
    text_rows(tg.at[far], far)
    take_weights(2, 2)

    def project(i, carry):
        rows = pl.ds(pl.multiple_of(i * 128, 128), 128)
        n = nrm[rows, :]
        both = jnp.dot(n, wg[0].reshape(1280, 1280), preferred_element_type=F32)
        qk[rows, :640] = (both[:, :640] + halved(qkvb, 0)).astype(BF)
        qk[rows, 640:] = (both[:, 640:] + halved(qkvb, 1280)).astype(BF)
        third = jnp.dot(n, wg[1, :, :, :640].reshape(1280, 640), preferred_element_type=F32)
        vv[rows, :] = (third + halved(qkvb, 2560)).astype(BF)
        return carry

    lax.fori_loop(0, 4, project, 0)
    for a in range(2):
        live = lax.broadcasted_iota(jnp.int32, (1, 256), 1) < facts[a][1]
        rows = slice(a * 256, a * 256 + 256)
        for h in range(8):
            q = qk[rows, h * 80 : h * 80 + 80]
            k = qk[rows, 640 + h * 80 : 640 + h * 80 + 80]
            val = vv[rows, h * 80 : h * 80 + 80]
            scores = lax.dot_general(
                q, k, (((1,), (1,)), ((), ())), preferred_element_type=F32
            ) * (1.0 / math.sqrt(80))
            scores = jnp.where(live, scores, NEG)
            weights = jnp.exp(scores - jnp.max(scores, axis=1, keepdims=True))
            prob = (weights / jnp.sum(weights, axis=1, keepdims=True)).astype(BF)
            ctx[rows, h * 80 : h * 80 + 80] = jnp.dot(
                prob, val, preferred_element_type=F32
            ).astype(BF)
    go(remote(ctx, ctxo, ess.at[0], ers.at[0], fp, s))

    def out_rows(owner):
        return wg[1, pl.ds(owner * 8, 8), :, 640:].reshape(640, 640)

    attended = jnp.dot(ctx[...], out_rows(core), preferred_element_type=F32)
    landed(ctxo, ers.at[0])
    attended = attended + jnp.dot(ctxo[...], out_rows(1 - core), preferred_element_type=F32)
    hidden = (st[:, lanes(0)].astype(F32) + attended + halved(outb, 0)).astype(BF)
    quarter = lax.broadcasted_iota(jnp.int32, (128, 512), 1) // 4 == lax.broadcasted_iota(
        jnp.int32, (128, 512), 0
    )
    pooled = jnp.dot(
        jnp.where(quarter, 0.25, 0.0).astype(BF), hidden, preferred_element_type=F32
    )
    pool[...] = pooled.astype(BF)
    go(remote(pool, poolo, ess.at[1], ers.at[1], fp, s))
    landed(poolo, ers.at[1])

    def square(c, total):
        cols = pl.ds(pl.multiple_of(c * 512, 128), 512)
        own_rows = pl.ds(pl.multiple_of(core * 640, 128), 640)
        other_rows = pl.ds(pl.multiple_of(640 - core * 640, 128), 640)
        seen = jnp.dot(pool[...], pw[own_rows, cols], preferred_element_type=F32)
        seen = seen + jnp.dot(poolo[...], pw[other_rows, cols], preferred_element_type=F32)
        seen = seen + prow[:, pl.ds(pl.multiple_of(c * 512, 128), 512)]
        return total + jnp.sum(seen * seen, axis=1, keepdims=True)

    prow[...] = pb
    total = lax.fori_loop(0, 8, square, jnp.zeros((128, 1), F32))
    scale = lax.rsqrt(total * (1.0 / 4096) + 1e-5)
    head = (pool[...].astype(F32) * scale).astype(BF)
    tail = jnp.where(lax.broadcasted_iota(jnp.int32, (128, 128), 1) == 0, scale, 0.0).astype(BF)
    want = lax.broadcasted_iota(jnp.int32, (128, 1), 0)
    frame_of = want // 4 % 2
    begin = jnp.where(frame_of == 0, facts[0][2], facts[1][2])
    token = (want // 8 - begin + 16384) % 16 + want % 4 * 16 + frame_of * 64
    taken = (token == lax.broadcasted_iota(jnp.int32, (128, 128), 1)).astype(F32).astype(BF)
    head = jnp.dot(taken, head, preferred_element_type=F32)
    tail = jnp.dot(taken, tail, preferred_element_type=F32)
    for i in range(16):
        tok[i, :, :640] = head[i * 8 : i * 8 + 8].astype(BF)
        tok[i, :, 640:] = tail[i * 8 : i * 8 + 8].astype(BF)
    for k in range(1, 16):
        go(remote(tok.at[seq_at(k)], land.at[s], sss.at[k], srs.at[k], f, seq_at(k)))
    land[s] = tok[s]
    for k in range(1, 16):
        landed(land.at[seq_at(16 - k)], srs.at[k])
    go(remote(land, table.at[f], xss.at[0], xrs.at[1], xs(1), s))
    go(remote(land, table.at[f], xss.at[1], xrs.at[3], xs(3), s))
    go(remote(land, table.at[f], pss.at[0], prs.at[0], fp, s))
    table[f] = land[...]
    for j in (1, 3):
        fs = xs(4 - j)
        landed(table.at[fs], xrs.at[j])
        part = table.at[fs, pl.ds(j // 2 * 8, 8)]
        go(remote(part, part, xss.at[2 + j // 2], fxr.at[j // 2], xs(j), s))
        go(remote(table.at[fs], table.at[fs], pss.at[j], prs.at[j], fp, s))
    for n in range(2):
        part = table.at[xs(2), pl.ds(n * 8, 8)]
        landed(part, fxr.at[n])
        go(remote(part, part, fps.at[n], fpr.at[n], fp, s))
    for j in (0, 1, 3):
        landed(table.at[(f // 2 + 4 - j) % 4 * 2 + 1 - core], prs.at[j])
    for n in range(2):
        landed(table.at[xs(2) + 1 - 2 * core, pl.ds(n * 8, 8)], fpr.at[n])
    parts = []
    for x in range(4):
        even = table[2 * x].astype(F32).reshape(128, 768).astype(BF)
        odd = table[2 * x + 1].astype(F32).reshape(128, 768).astype(BF)
        part = jnp.dot(even, fold[:768, :], preferred_element_type=F32)
        part = part + jnp.dot(odd, fold[768:, :], preferred_element_type=F32)
        parts.append(part.astype(BF))
    visual = jnp.concatenate(parts, axis=0)
    sign = jnp.where(lax.broadcasted_iota(jnp.int32, (1, 128), 1) < 64, -1.0, 1.0)
    factor = math.log2(math.e) / math.sqrt(128)
    for blk in range(4):
        some = slice(blk * 32, blk * 32 + 32)
        shape = (8, 32, 1)
        frame = lax.broadcasted_iota(jnp.int32, shape, 1) + blk * 32
        owner = lax.broadcasted_iota(jnp.int32, shape, 0)
        within = frame * 128 + owner * 16 + s - col[some, 1:2][None]
        live = (within >= 0) & (within < col[some, 2:3][None] // 4)
        source = jnp.where(live, col[some, 0:1][None] + within // 16, -1).reshape(256, 1)
        chosen = (source == lax.broadcasted_iota(jnp.int32, (256, 512), 1)).astype(F32).astype(BF)
        placed = jnp.dot(chosen, visual, preferred_element_type=F32)
        x = jnp.where(source >= 0, placed, plain[blk].reshape(256, 512))
        c1, s1 = trig[0, some, :][None], trig[1, some, :][None]
        c2, s2 = trig[0, 128:, :][:, None, :], trig[1, 128:, :][:, None, :]
        cosine = (c1 * c2 - s1 * s2).reshape(256, 128)
        sine = (s1 * c2 + c1 * s2).reshape(256, 128) * sign

        def rotate(n):
            part = x[:, n * 128 : n * 128 + 128]
            return part * cosine + pltpu.roll(part, 64, 1) * sine

        for h in range(2):
            q_out[blk, h * 256 : h * 256 + 256, :] = (rotate(h) * factor).astype(BF)
        rows = slice(blk % 2 * 256, blk % 2 * 256 + 256)
        kv_out[blk // 2, rows, :128] = rotate(2).astype(BF)
        kv_out[blk // 2, rows, 128:] = x[:, 384:].astype(BF)
    for n in range(2):
        landed(wo_half.at[n], ors.at[n])
    for copy in sends:
        copy.wait_send()


def front(rows, vmem_args, hbm_args):
    shape = jax.ShapeDtypeStruct
    dma = pltpu.SemaphoreType.DMA
    vmem = pl.BlockSpec(memory_space=pltpu.VMEM)
    hbm = pl.BlockSpec(memory_space=pl.ANY)
    buf = pltpu.VMEM
    return pl.pallas_call(
        front_kernel,
        out_shape=(
            shape((4, 512, 128), BF),
            shape((2, 512, 256), BF),
            shape((2, 128, 4096), BF),
        ),
        in_specs=[vmem] * (len(rows) + len(vmem_args)) + [hbm] * len(hbm_args),
        out_specs=(vmem, vmem, hbm),
        scratch_shapes=[
            buf((128, 4096), BF),
            buf((2, 80, 1280), BF),
            buf((2, 16, 80, 1280), BF),
            buf((2, 256, 1280), BF),
            buf((8, 128, 4096), BF),
            buf((1280, 4096), BF),
            buf((4096, 512), BF),
            buf((1536, 512), BF),
            buf((4, 8, 32, 512), F32),
            buf((512, 1280), BF),
            buf((512, 1280), BF),
            buf((512, 1280), BF),
            buf((512, 640), BF),
            buf((512, 640), BF),
            buf((512, 640), BF),
            buf((128, 640), BF),
            buf((128, 640), BF),
            buf((16, 8, 768), BF),
            buf((16, 8, 768), BF),
            buf((8, 16, 8, 768), BF),
            buf((128, 128), jnp.int32),
            buf((1, 4096), F32),
            dma((8,)),
            dma((2, 4, 4, 4)),
            dma((2, 4, 4, 2)),
            dma((4,)),
            dma((4,)),
            dma((3, 2)),
            dma((4, 2)),
            dma,
            dma,
            dma((2,)),
            dma((2,)),
            dma((16,)),
            dma((16,)),
            dma((4,)),
            dma((4,)),
            dma((4,)),
            dma((4,)),
            dma((2,)),
            dma((2,)),
            dma((2,)),
            dma((2,)),
            dma((2,)),
        ],
        compiler_params=pltpu.CompilerParams(
            collective_id=1, has_side_effects=True, vmem_limit_bytes=56 << 20
        ),
        name="front",
    )(*rows, *vmem_args, *hbm_args)


def attend(q_ref, acc, top, den, kv, tile, keys, base, inc):
    scores = lax.dot_general(
        q_ref[tile], kv[:keys, :128], (((1,), (1,)), ((), ())), preferred_element_type=F32
    )
    if base is not None:
        row = lax.broadcasted_iota(jnp.int32, (512, 1), 0) % 256
        col = lax.broadcasted_iota(jnp.int32, (1, keys), 1)
        row = row % 32 * 8 + row // 32 + base + inc
        col = col // 256 * 256 + col % 32 * 8 + col % 256 // 32
        scores = jnp.where(col < row, scores, NEG)
    old = top[tile]
    new = jnp.maximum(old, jnp.max(scores, axis=1, keepdims=True))
    fade = jnp.exp2(old - new)
    weights = jnp.exp2(scores - new[:, :1]).astype(BF)
    top[tile] = new
    wide = jnp.concatenate([kv[:keys, 128:], jnp.ones((keys, 128), BF)], axis=1)
    added = jnp.dot(weights, wide, preferred_element_type=F32)
    den[tile] = den[tile] * fade + added[:, 128:]
    acc[tile] = acc[tile] * fade + added[:, :128]


ORDER = (
    (0, 0), (1, 0), (3, 0), (2, 0), (0, 1), (0, 3), (1, 1), (1, 3),
    (0, 2), (3, 1), (3, 3), (1, 2), (2, 1), (2, 3), (3, 2), (2, 2),
)
TAKEN = {1: ((1, 0), (3, 0)), 2: (), 4: ((0, 1), (0, 3)), 5: ()}
PASSED = {1: (0,), 3: (1,), 4: (3,), 6: (2,)}
RELAYED = {1: ((1, 0), (3, 0)), 4: ((0, 1), (0, 3)), 5: ()}


def attention_kernel(
    q_far, own_far, wo, wo_half, out, q, own, kv, acc, top, den, ctx, seen, via, lhs, wog, give, got,
    local, ss, rs, css, crs, oss, ors, gss, grs,
):
    f, s, xs, ys, zs, fp = places()
    core = f % 2
    y, z = s // 4, s % 4
    brought = [
        pltpu.make_async_copy(own_far, own, local.at[4]),
        pltpu.make_async_copy(q_far, q, local.at[5]),
    ]
    for copy in brought:
        copy.start()
    greet(
        [(f, ys(1)), (f, ys(3)), (f, zs(1)), (f, zs(3))]
        + [(xs(k), s) for k in (1, 2, 3)]
        + [(fp, s)]
    )

    def slot_of(h, j, k):
        a, b = (4 - j) % 4, (4 - k) % 4
        if h == 0:
            return kv.at[0, ys(a) // 4 * 4 + zs(b) % 4]
        return kv.at[1, ys(b) // 4 * 4 + zs(a) % 4]

    def half_of(ref, n):
        return ref.at[pl.ds(n * 256, 256)]

    def kv_copy(h, j, k, n, a, b, at, to):
        return remote(a, b, ss.at[h, j, k, n], rs.at[(h,) + at], f, to)

    def start_copies():
        result = []
        for h in range(2):
            first = (ys, zs)[h]
            slot = slot_of(h, 0, 0)
            result.append(kv_copy(h, 0, 0, 0, own.at[h], slot, (1, 0, 0), first(1)))
            result.append(kv_copy(h, 0, 0, 1, own.at[h], slot, (3, 0, 0), first(3)))
        return result

    def pass_copies(j):
        result = []
        for h in range(2):
            second = (zs, ys)[h]
            slot = slot_of(h, j, 0)
            full = own.at[h] if j == 0 else slot
            result.append(kv_copy(h, j, 0, 2, full, slot, (j, 1, 0), second(1)))
            result.append(kv_copy(h, j, 0, 3, full, slot, (j, 3, 0), second(3)))
        return result

    def relay_copies(j, k):
        result = []
        for h in range(2):
            first, second = (ys, zs) if h == 0 else (zs, ys)
            n, at, to = (j // 2, (2, 0), first(j)) if k == 0 else (k // 2, (j, 2), second(k))
            part = half_of(slot_of(h, j, k), n)
            result.append(kv_copy(h, j, k, 0, part, part, at + (n,), to))
        return result

    def copies_at(n):
        j, k = ORDER[n]
        relayed = RELAYED.get(n, ((j, k),) if k in (1, 3) else ())
        result = []
        for jj, kk in relayed:
            result += relay_copies(jj, kk)
        for jj in PASSED.get(n, ()):
            result += pass_copies(jj)
        return result

    def landed(dst, recv):
        remote(dst, dst, local.at[0], recv, fp, s).wait_recv()

    def take(j, k):
        for h in range(2):
            slot = slot_of(h, j, k)
            if k == 2 or (j == 2 and k == 0):
                landed(half_of(slot, 0), rs.at[h, j, k, 0])
                landed(half_of(slot, 1), rs.at[h, j, k, 1])
            else:
                landed(slot, rs.at[h, j, k, 0])

    for copy in brought:
        copy.wait()
    for copy in start_copies():
        copy.start()
    lower, upper = pl.ds(0, 128), pl.ds(128, 128)
    parts = [
        remote(wo_half.at[0], wog.at[2, lower], oss.at[0], ors.at[0], xs(1), s),
        remote(wo_half.at[1], wog.at[2, upper], oss.at[1], ors.at[1], xs(3), s),
        remote(wo.at[upper], wog.at[3, upper], oss.at[2], ors.at[2], xs(1), s),
        remote(wo.at[lower], wog.at[1, lower], oss.at[3], ors.at[3], xs(3), s),
    ]
    keeps = [
        pltpu.make_async_copy(wo, wog.at[0], local.at[1]),
        pltpu.make_async_copy(wo_half.at[0], wog.at[3, lower], local.at[2]),
        pltpu.make_async_copy(wo_half.at[1], wog.at[1, upper], local.at[3]),
    ]
    for copy in parts + keeps:
        copy.start()
    kv[0, s] = own[0]
    kv[1, s] = own[1]
    top[...] = jnp.full_like(top, NEG)
    den[...] = jnp.zeros_like(den)
    acc[...] = jnp.zeros_like(acc)

    def step(i, carry):
        j = k = 0
        for n, (jj, kk) in enumerate(ORDER):
            if n > 0:
                j = jnp.where(i == n, jj, j)
                k = jnp.where(i == n, kk, k)

                @pl.when(i == n)
                def _(n=n, jj=jj, kk=kk):
                    for at in TAKEN.get(n, ((jj, kk),)):
                        take(*at)
                    for copy in copies_at(n):
                        copy.start()

        a = (y + 4 - j) % 4 * 4 + (z + 4 - k) % 4
        b = (y + 4 - k) % 4 * 4 + (z + 4 - j) % 4
        at = functools.partial(attend, q, acc, top, den)
        inc = jnp.where(a <= s, 1, 0)
        at(kv.at[0, a], 0, 256, 0, inc)
        at(kv.at[0, a], 1, 512, 256, inc)
        at(kv.at[0, a], 2, 512, None, inc)
        at(kv.at[0, a], 3, 512, None, inc)
        inc = jnp.where(b <= s, 1, 0)
        at(kv.at[1, b], 2, 256, 0, inc)
        at(kv.at[1, b], 3, 512, 256, inc)
        return carry

    lax.fori_loop(0, 16, step, 0)
    for tile in range(4):
        block = (acc[tile] / den[tile]).astype(BF)
        for head in range(2):
            for owner in range(8):
                start = head * 256 + owner * 32
                ctx[owner // 2, owner % 2, tile, head] = block[start : start + 32]
    for copy in start_copies():
        copy.wait_send()
    for n in range(1, 16):
        for copy in copies_at(n):
            copy.wait_send()
    x = f // 2
    far = (x + 2) % 4
    last = [
        remote(ctx.at[far, 0], via.at[0], css.at[0], crs.at[0], xs(1), s),
        remote(ctx.at[far, 1], via.at[1], css.at[1], crs.at[1], xs(3), s),
        remote(ctx.at[(x + 1) % 4], seen.at[3], css.at[2], crs.at[2], xs(1), s),
        remote(ctx.at[(x + 3) % 4], seen.at[1], css.at[3], crs.at[3], xs(3), s),
        remote(via.at[0], seen.at[2, 0], css.at[4], crs.at[4], xs(1), s),
        remote(via.at[1], seen.at[2, 1], css.at[5], crs.at[5], xs(3), s),
    ]
    for copy in last[:4]:
        copy.start()
    seen[0] = ctx[x]
    for n in range(2):
        landed(via.at[n], crs.at[n])
        last[4 + n].start()
    for copy in keeps:
        copy.wait()
    for copy in parts:
        copy.wait()
    landed(seen.at[3], crs.at[2])
    landed(seen.at[1], crs.at[3])
    landed(seen.at[2, 0], crs.at[4])
    landed(seen.at[2, 1], crs.at[5])
    for d in range(4):
        for head in range(2):
            cols = slice(d * 256 + head * 128, d * 256 + head * 128 + 128)
            for owner in range(2):
                lhs[owner, :, cols] = seen[d, owner, :, head].reshape(128, 128)

    def columns(c):
        return pl.ds(pl.multiple_of(c * 512, 128), 512)

    def share(c):
        return remote(
            give.at[:, columns(c)], got.at[:, columns(c)], gss.at[c], grs.at[c], fp, s
        )

    def partial(owner, c):
        return jnp.dot(
            lhs[owner], wog[:, :, columns(c)].reshape(1024, 512), preferred_element_type=F32
        )

    def to_partner(c, carry):
        give[:, columns(c)] = partial(1 - core, c).astype(BF)

        @pl.when(c > 0)
        def _():
            share(c - 1).start()

        return carry

    def to_output(c, carry):
        mine = partial(core, c)

        @pl.when(c == 0)
        def _():
            share(7).start()

        share(c).wait()
        out[:, columns(c)] = (mine + got[:, columns(c)].astype(F32)).astype(BF)
        return carry

    lax.fori_loop(0, 8, to_partner, 0)
    lax.fori_loop(0, 8, to_output, 0)
    for copy in last:
        copy.wait_send()


def attention(q, own, wo, wo_half):
    dma = pltpu.SemaphoreType.DMA
    vmem = pl.BlockSpec(memory_space=pltpu.VMEM)
    hbm = pl.BlockSpec(memory_space=pl.ANY)
    state = pltpu.VMEM((4, 512, 128), F32)
    return pl.pallas_call(
        attention_kernel,
        out_shape=jax.ShapeDtypeStruct((128, 4096), BF),
        in_specs=[hbm] * 4,
        out_specs=vmem,
        scratch_shapes=[
            pltpu.VMEM((4, 512, 128), BF),
            pltpu.VMEM((2, 512, 256), BF),
            pltpu.VMEM((2, 16, 512, 256), BF),
            state,
            state,
            state,
            pltpu.VMEM((4, 2, 4, 2, 32, 128), BF),
            pltpu.VMEM((4, 2, 4, 2, 32, 128), BF),
            pltpu.VMEM((2, 4, 2, 32, 128), BF),
            pltpu.VMEM((2, 128, 1024), BF),
            pltpu.VMEM((4, 256, 4096), BF),
            pltpu.VMEM((128, 4096), BF),
            pltpu.VMEM((128, 4096), BF),
            dma((6,)),
            dma((2, 4, 4, 4)),
            dma((2, 4, 4, 2)),
            dma((6,)),
            dma((6,)),
            dma((4,)),
            dma((4,)),
            dma((8,)),
            dma((8,)),
        ],
        compiler_params=pltpu.CompilerParams(
            collective_id=3, has_side_effects=True, vmem_limit_bytes=48 << 20
        ),
        name="attention",
    )(q, own, wo, wo_half)


def per_device(
    vit_states,
    frame_slot,
    patch_count,
    vis_start,
    text_embed,
    vit_ln_gain,
    vit_ln_bias,
    vit_qkv_w,
    vit_qkv_b,
    vit_out_w,
    vit_out_b,
    proj_w,
    proj_b,
    attn_gain,
    wq,
    wk,
    wv,
    wo,
):
    s = lax.axis_index("seq")
    exponents = jnp.arange(0, 128, 2).astype(F32) / 128
    inverse = jnp.power(F32(ROPE_THETA), -exponents)
    steps = jnp.concatenate([jnp.arange(128) * 128, jnp.arange(8) * 16 + s]).astype(F32)
    angles = steps[:, None] * jnp.concatenate([inverse, inverse])[None, :]
    trig = jnp.stack([jnp.cos(angles), jnp.sin(angles)])
    queries, own, wo_half = front(
        [frame_slot[None], patch_count[None], vis_start[None]],
        [
            vit_states,
            vit_qkv_w,
            vit_out_w,
            text_embed.reshape(128, 4096),
            vit_ln_gain,
            vit_ln_bias,
            vit_out_b,
            vit_qkv_b,
            proj_b,
            attn_gain,
            trig,
        ],
        [proj_w, wq, wk, wv, wo],
    )
    return attention(queries, own, wo, wo_half).reshape(128, 1, 4096)


def solution(mesh):
    return jax.shard_map(
        per_device,
        mesh=mesh,
        in_specs=(
            P(("frame", "seq"), None, None),
            P(),
            P(),
            P(),
            P(None, ("frame", "seq"), None),
            P(),
            P(),
            P("seq", None),
            P(),
            P("seq", None),
            P(),
            P(),
            P(),
            P(),
            P(None, "frame"),
            P(None, "frame"),
            P(None, "frame"),
            P("frame", None),
        ),
        out_specs=P(None, ("frame", "seq"), None),
        check_vma=False,
    )
```

```python
import functools
import math

import jax
import jax.numpy as jnp
from jax import lax
from jax.experimental import pallas as pl
from jax.experimental.pallas import tpu as pltpu
from jax.sharding import PartitionSpec as P

MESH = pl.DeviceIdType.MESH
BF = jnp.bfloat16
F32 = jnp.float32
NEG = -1e30
ROPE_THETA = 500000.0
NEAR_FIRST = (1, 3, 2)


def remote(src, dst, send, recv, f, s):
    return pltpu.make_async_remote_copy(
        src_ref=src,
        dst_ref=dst,
        send_sem=send,
        recv_sem=recv,
        device_id={"frame": f, "seq": s},
        device_id_type=MESH,
    )


def places():
    f = lax.axis_index("frame")
    s = lax.axis_index("seq")
    y, z = s // 4, s % 4

    def along_y(k):
        return (y + k) % 4 * 4 + z

    def along_z(k):
        return y * 4 + (z + k) % 4

    def along_x(k):
        return (f // 2 + k) % 4 * 2 + f % 2

    partner = f + 1 - 2 * (f % 2)
    return f, s, along_x, along_y, along_z, partner


def greet(peers):
    barrier = pltpu.get_barrier_semaphore()
    for f, s in peers:
        pl.semaphore_signal(
            barrier, inc=1, device_id={"frame": f, "seq": s}, device_id_type=MESH
        )
    pl.semaphore_wait(barrier, len(peers))


def turned(row, eye):
    return jnp.sum(jnp.where(eye, row.astype(F32), 0.0), axis=1, keepdims=True).astype(jnp.int32)


def front_kernel(
    slot_r, count_r, start_r, v, qkvw, outw, t_raw, ln_gr, ln_br, outb, qkvb, pbr, gainr, trig,
    proj, wq, wk, wv, wo,
    q_out, kv_out, wo_half,
    t, ws, wg, vp, tg, pw, wc, fold, plain, st, nrm, qk, vv, ctx, ctxo, pool, poolo, tok, land, table, col, prow,
    local, wss, wrs, tss, trs, hss, hrs, vss, vrs, ess, ers, sss, srs, xss, xrs, pss, prs, oss, ors, fxr, fps, fpr,
):
    f, s, xs, ys, zs, fp = places()
    core = f % 2

    def seq_at(k):
        return (s + k) % 16

    def lanes(first):
        return pl.ds(pl.multiple_of(first + core * 640, 128), 640)

    def halved(ref, first):
        row = ref[...][None]
        return jnp.where(
            core == 0, row[:, first : first + 640], row[:, first + 640 : first + 1280]
        )

    def landed(dst, recv):
        remote(dst, dst, vss, recv, fp, s).wait_recv()

    ln_g, ln_b = ln_gr[...][None], ln_br[...][None]
    pb, again = pbr[...][None], gainr[...][None]
    packs = [
        pltpu.make_async_copy(qkvw.at[:, lanes(0)], ws.at[0, :, pl.ds(0, 640)], local.at[0]),
        pltpu.make_async_copy(qkvw.at[:, lanes(1280)], ws.at[0, :, pl.ds(640, 640)], local.at[1]),
        pltpu.make_async_copy(qkvw.at[:, lanes(2560)], ws.at[1, :, pl.ds(0, 640)], local.at[2]),
        pltpu.make_async_copy(outw.at[:, lanes(0)], ws.at[1, :, pl.ds(640, 640)], local.at[3]),
    ]
    loads = [
        pltpu.make_async_copy(wq, wc.at[:, pl.ds(0, 256)], local.at[4]),
        pltpu.make_async_copy(wk, wc.at[:, pl.ds(256, 128)], local.at[5]),
        pltpu.make_async_copy(wv, wc.at[:, pl.ds(384, 128)], local.at[6]),
        pltpu.make_async_copy(proj, pw, local.at[7]),
    ]
    for copy in packs + loads:
        copy.start()
    for i in range(4):
        rows = slice(i * 32, i * 32 + 32)
        x = t_raw[rows, :].astype(F32)
        x = x * lax.rsqrt(jnp.mean(x * x, axis=1, keepdims=True) + 1e-5)
        t[rows, :] = (x * again).astype(BF)
    greet(
        [(f, seq_at(k)) for k in range(1, 16)]
        + [(xs(k), s) for k in (1, 2, 3)]
        + [(fp, s)]
    )
    for copy in packs:
        copy.wait()
    sends = []

    def go(copy):
        copy.start()
        sends.append(copy)

    def weight_slot(h, j, k):
        a, b = (4 - j) % 4, (4 - k) % 4
        if h == 0:
            return wg.at[0, ys(a) // 4 * 4 + zs(b) % 4]
        return wg.at[1, ys(b) // 4 * 4 + zs(a) % 4]

    def weight_half(ref, n):
        return ref.at[:, pl.ds(n * 640, 640)]

    def weight_copy(h, j, k, n, a, b, at, to):
        go(remote(a, b, wss.at[h, j, k, n], wrs.at[(h,) + at], f, to))

    def start_weights():
        for h in range(2):
            first = (ys, zs)[h]
            slot = weight_slot(h, 0, 0)
            weight_copy(h, 0, 0, 0, ws.at[h], slot, (1, 0, 0), first(1))
            weight_copy(h, 0, 0, 1, ws.at[h], slot, (3, 0, 0), first(3))

    def pass_weights(j):
        for h in range(2):
            second = (zs, ys)[h]
            slot = weight_slot(h, j, 0)
            full = ws.at[h] if j == 0 else slot
            weight_copy(h, j, 0, 2, full, slot, (j, 1, 0), second(1))
            weight_copy(h, j, 0, 3, full, slot, (j, 3, 0), second(3))

    def relay_weights(j, k):
        for h in range(2):
            first, second = (ys, zs) if h == 0 else (zs, ys)
            n, at, to = (j // 2, (2, 0), first(j)) if k == 0 else (k // 2, (j, 2), second(k))
            part = weight_half(weight_slot(h, j, k), n)
            weight_copy(h, j, k, 0, part, part, at + (n,), to)

    def take_weights(j, k):
        for h in range(2):
            slot = weight_slot(h, j, k)
            if k == 2 or (j == 2 and k == 0):
                landed(weight_half(slot, 0), wrs.at[h, j, k, 0])
                landed(weight_half(slot, 1), wrs.at[h, j, k, 1])
            else:
                landed(slot, wrs.at[h, j, k, 0])
        if k in (1, 3):
            relay_weights(j, k)

    start_weights()
    go(remote(v, vp, vss, vrs, fp, s))
    go(remote(t, tg.at[f], tss.at[0], trs.at[1], xs(1), s))
    go(remote(t, tg.at[f], tss.at[1], trs.at[3], xs(3), s))
    go(remote(t, tg.at[f], hss.at[0, 0], hrs.at[0, 0], fp, s))
    wg[0, s] = ws[0]
    wg[1, s] = ws[1]
    slot = slot_r[...]
    holder = slot // 2
    pair = holder // 32 * 16 + holder % 16
    order = holder // 16 % 2 * 2 + slot % 2
    eye = lax.broadcasted_iota(jnp.int32, (128, 128), 0) == lax.broadcasted_iota(
        jnp.int32, (128, 128), 1
    )
    pair_c, order_c = turned(pair, eye), turned(order, eye)
    same = pair_c == pair
    rank = jnp.sum(jnp.where(same & (order_c < order), 1.0, 0.0), axis=0, keepdims=True).astype(
        jnp.int32
    )
    col[:, 0:1] = pair_c * 8 + turned(rank, eye) * 4
    col[:, 1:2] = turned(start_r[...], eye)
    col[:, 2:3] = turned(count_r[...], eye)
    facts = []
    for a in range(2):
        mine = (pair == f // 2 * 16 + s) & (rank == a)
        facts.append(
            [
                jnp.sum(
                    jnp.where(mine, row.astype(F32), 0.0), axis=1, keepdims=True
                ).astype(jnp.int32)
                for row in (order, count_r[...], start_r[...])
            ]
        )
    for copy in loads:
        copy.wait()

    def fold_rows(i, carry):
        rows = pl.ds(pl.multiple_of(i * 128, 128), 128)
        to = pl.ds(pl.multiple_of(i * 128 + i // 5 * 128, 128), 128)
        gained = (pw[rows, :].astype(F32) * again).astype(BF)
        fold[to, :] = jnp.dot(gained, wc[...], preferred_element_type=F32).astype(BF)
        return carry

    def text_rows(source, at):
        plain[:, at] = jnp.dot(source[...], wc[...], preferred_element_type=F32).reshape(4, 32, 512)

    def text_half(ref, n):
        return ref.at[pl.ds(n * 64, 64)]

    lax.fori_loop(0, 3, fold_rows, 0)
    take_weights(1, 0)
    take_weights(3, 0)
    relay_weights(1, 0)
    relay_weights(3, 0)
    pass_weights(0)
    lax.fori_loop(3, 6, fold_rows, 0)
    pass_weights(1)
    lax.fori_loop(6, 8, fold_rows, 0)
    take_weights(2, 0)
    pass_weights(2)
    pass_weights(3)
    take_weights(0, 1)
    take_weights(0, 3)
    lax.fori_loop(8, 10, fold_rows, 0)
    row = lax.broadcasted_iota(jnp.int32, (16, 1), 0)
    biased = pb * again
    upper = biased.astype(BF).astype(F32)
    biased = jnp.where(row == 0, upper, jnp.where(row == 1, biased - upper, 0.0)).astype(BF)
    biased = jnp.dot(biased, wc[...], preferred_element_type=F32)
    biased = jnp.sum(biased, axis=0, keepdims=True)
    first = lax.broadcasted_iota(jnp.int32, (128, 512), 0) == 0
    fold[640:768, :] = jnp.where(first, biased, 0.0).astype(BF)
    fold[1408:1536, :] = jnp.zeros((128, 512), BF)
    text_rows(t, f)
    take_weights(1, 1)
    take_weights(1, 3)
    landed(vp, vrs)
    for a in range(2):
        pick = facts[a][0]
        chosen = jnp.zeros((256, 1280), F32)
        for n in range(2):
            chosen = jnp.where(pick == core * 2 + n, v[n].astype(F32), chosen)
            chosen = jnp.where(pick == 2 - core * 2 + n, vp[n].astype(F32), chosen)
        st[a * 256 : a * 256 + 256, :] = chosen.astype(BF)

    def norm_rows(i, carry):
        rows = pl.ds(pl.multiple_of(i * 128, 128), 128)
        x = st[rows, :].astype(F32)
        centred = x - jnp.mean(x, axis=1, keepdims=True)
        spread = jnp.mean(centred * centred, axis=1, keepdims=True)
        nrm[rows, :] = (centred * lax.rsqrt(spread + 1e-6) * ln_g + ln_b).astype(BF)
        return carry

    lax.fori_loop(0, 4, norm_rows, 0)
    for j in (1, 3):
        fs = xs(4 - j)
        here = tg.at[fs]
        landed(here, trs.at[j])
        part = text_half(here, j // 2)
        go(remote(part, part, tss.at[2 + j // 2], hrs.at[2, j // 2], xs(j), s))
        go(remote(here, here, hss.at[1, j // 2], hrs.at[1, j // 2], fp, s))
    for n in range(2):
        half = pl.ds(n * 128, 128)
        go(remote(wo.at[half], wo_half.at[n], oss.at[n], ors.at[n], xs(1 + 2 * n), s))
    take_weights(2, 1)
    take_weights(2, 3)
    text_rows(tg.at[xs(3)], xs(3))
    take_weights(3, 1)
    take_weights(3, 3)
    text_rows(tg.at[xs(1)], xs(1))
    landed(tg.at[fp], hrs.at[0, 0])
    text_rows(tg.at[fp], fp)
    take_weights(0, 2)
    for j in (1, 3):
        fs = xs(4 - j) + 1 - 2 * core
        landed(tg.at[fs], hrs.at[1, j // 2])
        text_rows(tg.at[fs], fs)
    take_weights(1, 2)
    take_weights(3, 2)
    far = xs(2)
    for n in range(2):
        part = text_half(tg.at[far], n)
        landed(part, hrs.at[2, n])
        go(remote(part, part, hss.at[2, n], hrs.at[3, n], fp, s))
    text_rows(tg.at[far], far)
    far = far + 1 - 2 * core
    for n in range(2):
        landed(text_half(tg.at[far], n), hrs.at[3, n])
    text_rows(tg.at[far], far)
    take_weights(2, 2)

    def project(i, carry):
        rows = pl.ds(pl.multiple_of(i * 128, 128), 128)
        n = nrm[rows, :]
        both = jnp.dot(n, wg[0].reshape(1280, 1280), preferred_element_type=F32)
        qk[rows, :640] = (both[:, :640] + halved(qkvb, 0)).astype(BF)
        qk[rows, 640:] = (both[:, 640:] + halved(qkvb, 1280)).astype(BF)
        third = jnp.dot(n, wg[1, :, :, :640].reshape(1280, 640), preferred_element_type=F32)
        vv[rows, :] = (third + halved(qkvb, 2560)).astype(BF)
        return carry

    lax.fori_loop(0, 4, project, 0)
    for a in range(2):
        live = lax.broadcasted_iota(jnp.int32, (1, 256), 1) < facts[a][1]
        rows = slice(a * 256, a * 256 + 256)
        for h in range(8):
            q = qk[rows, h * 80 : h * 80 + 80]
            k = qk[rows, 640 + h * 80 : 640 + h * 80 + 80]
            val = vv[rows, h * 80 : h * 80 + 80]
            scores = lax.dot_general(
                q, k, (((1,), (1,)), ((), ())), preferred_element_type=F32
            ) * (math.log2(math.e) / math.sqrt(80))
            scores = jnp.where(live, scores, NEG)
            weights = jnp.exp2(scores - jnp.max(scores, axis=1, keepdims=True))
            prob = (weights * (1.0 / jnp.sum(weights, axis=1, keepdims=True))).astype(BF)
            ctx[rows, h * 80 : h * 80 + 80] = jnp.dot(
                prob, val, preferred_element_type=F32
            ).astype(BF)
    go(remote(ctx, ctxo, ess.at[0], ers.at[0], fp, s))

    def out_rows(owner):
        return wg[1, pl.ds(owner * 8, 8), :, 640:].reshape(640, 640)

    attended = jnp.dot(ctx[...], out_rows(core), preferred_element_type=F32)
    landed(ctxo, ers.at[0])
    attended = attended + jnp.dot(ctxo[...], out_rows(1 - core), preferred_element_type=F32)
    hidden = (st[:, lanes(0)].astype(F32) + attended + halved(outb, 0)).astype(BF)
    quarter = lax.broadcasted_iota(jnp.int32, (128, 512), 1) // 4 == lax.broadcasted_iota(
        jnp.int32, (128, 512), 0
    )
    pooled = jnp.dot(
        jnp.where(quarter, 0.25, 0.0).astype(BF), hidden, preferred_element_type=F32
    )
    pool[...] = pooled.astype(BF)
    go(remote(pool, poolo, ess.at[1], ers.at[1], fp, s))
    landed(poolo, ers.at[1])

    def square(c, total):
        cols = pl.ds(pl.multiple_of(c * 512, 128), 512)
        own_rows = pl.ds(pl.multiple_of(core * 640, 128), 640)
        other_rows = pl.ds(pl.multiple_of(640 - core * 640, 128), 640)
        seen = jnp.dot(pool[...], pw[own_rows, cols], preferred_element_type=F32)
        seen = seen + jnp.dot(poolo[...], pw[other_rows, cols], preferred_element_type=F32)
        seen = seen + prow[:, pl.ds(pl.multiple_of(c * 512, 128), 512)]
        return total + jnp.sum(seen * seen, axis=1, keepdims=True)

    prow[...] = pb
    total = lax.fori_loop(0, 8, square, jnp.zeros((128, 1), F32))
    scale = lax.rsqrt(total * (1.0 / 4096) + 1e-5)
    head = (pool[...].astype(F32) * scale).astype(BF)
    tail = jnp.where(lax.broadcasted_iota(jnp.int32, (128, 128), 1) == 0, scale, 0.0).astype(BF)
    want = lax.broadcasted_iota(jnp.int32, (128, 1), 0)
    frame_of = want // 4 % 2
    begin = jnp.where(frame_of == 0, facts[0][2], facts[1][2])
    token = (want // 8 - begin + 16384) % 16 + want % 4 * 16 + frame_of * 64
    taken = (token == lax.broadcasted_iota(jnp.int32, (128, 128), 1)).astype(F32).astype(BF)
    head = jnp.dot(taken, head, preferred_element_type=F32)
    tail = jnp.dot(taken, tail, preferred_element_type=F32)
    for i in range(16):
        tok[i, :, :640] = head[i * 8 : i * 8 + 8].astype(BF)
        tok[i, :, 640:] = tail[i * 8 : i * 8 + 8].astype(BF)
    for k in range(1, 16):
        go(remote(tok.at[seq_at(k)], land.at[s], sss.at[k], srs.at[k], f, seq_at(k)))
    land[s] = tok[s]
    for k in range(1, 16):
        landed(land.at[seq_at(16 - k)], srs.at[k])
    go(remote(land, table.at[f], xss.at[0], xrs.at[1], xs(1), s))
    go(remote(land, table.at[f], xss.at[1], xrs.at[3], xs(3), s))
    go(remote(land, table.at[f], pss.at[0], prs.at[0], fp, s))
    table[f] = land[...]
    for j in (1, 3):
        fs = xs(4 - j)
        landed(table.at[fs], xrs.at[j])
        part = table.at[fs, pl.ds(j // 2 * 8, 8)]
        go(remote(part, part, xss.at[2 + j // 2], fxr.at[j // 2], xs(j), s))
        go(remote(table.at[fs], table.at[fs], pss.at[j], prs.at[j], fp, s))
    for n in range(2):
        part = table.at[xs(2), pl.ds(n * 8, 8)]
        landed(part, fxr.at[n])
        go(remote(part, part, fps.at[n], fpr.at[n], fp, s))
    for j in (0, 1, 3):
        landed(table.at[(f // 2 + 4 - j) % 4 * 2 + 1 - core], prs.at[j])
    for n in range(2):
        landed(table.at[xs(2) + 1 - 2 * core, pl.ds(n * 8, 8)], fpr.at[n])
    parts = []
    for x in range(4):
        even = table[2 * x].astype(F32).reshape(128, 768).astype(BF)
        odd = table[2 * x + 1].astype(F32).reshape(128, 768).astype(BF)
        part = jnp.dot(even, fold[:768, :], preferred_element_type=F32)
        part = part + jnp.dot(odd, fold[768:, :], preferred_element_type=F32)
        parts.append(part.astype(BF))
    visual = jnp.concatenate(parts, axis=0)
    sign = jnp.where(lax.broadcasted_iota(jnp.int32, (1, 128), 1) < 64, -1.0, 1.0)
    factor = math.log2(math.e) / math.sqrt(128)
    for blk in range(4):
        some = slice(blk * 32, blk * 32 + 32)
        shape = (8, 32, 1)
        frame = lax.broadcasted_iota(jnp.int32, shape, 1) + blk * 32
        owner = lax.broadcasted_iota(jnp.int32, shape, 0)
        within = frame * 128 + owner * 16 + s - col[some, 1:2][None]
        live = (within >= 0) & (within < col[some, 2:3][None] // 4)
        source = jnp.where(live, col[some, 0:1][None] + within // 16, -1).reshape(256, 1)
        chosen = (source == lax.broadcasted_iota(jnp.int32, (256, 512), 1)).astype(F32).astype(BF)
        placed = jnp.dot(chosen, visual, preferred_element_type=F32)
        x = jnp.where(source >= 0, placed, plain[blk].reshape(256, 512))
        c1, s1 = trig[0, some, :][None], trig[1, some, :][None]
        c2, s2 = trig[0, 128:, :][:, None, :], trig[1, 128:, :][:, None, :]
        cosine = (c1 * c2 - s1 * s2).reshape(256, 128)
        sine = (s1 * c2 + c1 * s2).reshape(256, 128) * sign

        def rotate(n):
            part = x[:, n * 128 : n * 128 + 128]
            return part * cosine + pltpu.roll(part, 64, 1) * sine

        for h in range(2):
            q_out[blk, h * 256 : h * 256 + 256, :] = (rotate(h) * factor).astype(BF)
        rows = slice(blk % 2 * 256, blk % 2 * 256 + 256)
        kv_out[blk // 2, rows, :128] = rotate(2).astype(BF)
        kv_out[blk // 2, rows, 128:] = x[:, 384:].astype(BF)
    for n in range(2):
        landed(wo_half.at[n], ors.at[n])
    for copy in sends:
        copy.wait_send()


def front(rows, vmem_args, hbm_args):
    shape = jax.ShapeDtypeStruct
    dma = pltpu.SemaphoreType.DMA
    vmem = pl.BlockSpec(memory_space=pltpu.VMEM)
    hbm = pl.BlockSpec(memory_space=pl.ANY)
    buf = pltpu.VMEM
    return pl.pallas_call(
        front_kernel,
        out_shape=(
            shape((4, 512, 128), BF),
            shape((2, 512, 256), BF),
            shape((2, 128, 4096), BF),
        ),
        in_specs=[vmem] * (len(rows) + len(vmem_args)) + [hbm] * len(hbm_args),
        out_specs=(vmem, vmem, hbm),
        scratch_shapes=[
            buf((128, 4096), BF),
            buf((2, 80, 1280), BF),
            buf((2, 16, 80, 1280), BF),
            buf((2, 256, 1280), BF),
            buf((8, 128, 4096), BF),
            buf((1280, 4096), BF),
            buf((4096, 512), BF),
            buf((1536, 512), BF),
            buf((4, 8, 32, 512), F32),
            buf((512, 1280), BF),
            buf((512, 1280), BF),
            buf((512, 1280), BF),
            buf((512, 640), BF),
            buf((512, 640), BF),
            buf((512, 640), BF),
            buf((128, 640), BF),
            buf((128, 640), BF),
            buf((16, 8, 768), BF),
            buf((16, 8, 768), BF),
            buf((8, 16, 8, 768), BF),
            buf((128, 128), jnp.int32),
            buf((1, 4096), F32),
            dma((8,)),
            dma((2, 4, 4, 4)),
            dma((2, 4, 4, 2)),
            dma((4,)),
            dma((4,)),
            dma((3, 2)),
            dma((4, 2)),
            dma,
            dma,
            dma((2,)),
            dma((2,)),
            dma((16,)),
            dma((16,)),
            dma((4,)),
            dma((4,)),
            dma((4,)),
            dma((4,)),
            dma((2,)),
            dma((2,)),
            dma((2,)),
            dma((2,)),
            dma((2,)),
        ],
        compiler_params=pltpu.CompilerParams(
            collective_id=1, has_side_effects=True, vmem_limit_bytes=56 << 20
        ),
        name="front",
    )(*rows, *vmem_args, *hbm_args)


def attend(q_ref, acc, top, den, kv, tile, keys, base, inc):
    scores = lax.dot_general(
        q_ref[tile], kv[:keys, :128], (((1,), (1,)), ((), ())), preferred_element_type=F32
    )
    if base is not None:
        row = lax.broadcasted_iota(jnp.int32, (512, 1), 0) % 256
        col = lax.broadcasted_iota(jnp.int32, (1, keys), 1)
        row = row % 32 * 8 + row // 32 + base + inc
        col = col // 256 * 256 + col % 32 * 8 + col % 256 // 32
        scores = jnp.where(col < row, scores, NEG)
    old = top[tile]
    new = jnp.maximum(old, jnp.max(scores, axis=1, keepdims=True))
    fade = jnp.exp2(old - new)
    weights = jnp.exp2(scores - new[:, :1]).astype(BF)
    top[tile] = new
    wide = jnp.concatenate([kv[:keys, 128:], jnp.ones((keys, 128), BF)], axis=1)
    added = jnp.dot(weights, wide, preferred_element_type=F32)
    den[tile] = den[tile] * fade + added[:, 128:]
    acc[tile] = acc[tile] * fade + added[:, :128]


ORDER = (
    (0, 0), (1, 0), (3, 0), (2, 0), (0, 1), (0, 3), (1, 1), (1, 3),
    (0, 2), (3, 1), (3, 3), (1, 2), (2, 1), (2, 3), (3, 2), (2, 2),
)
TAKEN = {1: ((1, 0), (3, 0)), 2: (), 4: ((0, 1), (0, 3)), 5: ()}
PASSED = {1: (0,), 3: (1,), 4: (3,), 6: (2,)}
RELAYED = {1: ((1, 0), (3, 0)), 4: ((0, 1), (0, 3)), 5: ()}


def attention_kernel(
    q_far, own_far, wo, wo_half, out, q, own, kv, acc, top, den, ctx, seen, via, lhs, wog, give, got,
    local, ss, rs, css, crs, oss, ors, gss, grs,
):
    f, s, xs, ys, zs, fp = places()
    core = f % 2
    y, z = s // 4, s % 4
    brought = [
        pltpu.make_async_copy(own_far, own, local.at[4]),
        pltpu.make_async_copy(q_far, q, local.at[5]),
    ]
    for copy in brought:
        copy.start()
    greet(
        [(f, ys(1)), (f, ys(3)), (f, zs(1)), (f, zs(3))]
        + [(xs(k), s) for k in (1, 2, 3)]
        + [(fp, s)]
    )

    def slot_of(h, j, k):
        a, b = (4 - j) % 4, (4 - k) % 4
        if h == 0:
            return kv.at[0, ys(a) // 4 * 4 + zs(b) % 4]
        return kv.at[1, ys(b) // 4 * 4 + zs(a) % 4]

    def half_of(ref, n):
        return ref.at[pl.ds(n * 256, 256)]

    def kv_copy(h, j, k, n, a, b, at, to):
        return remote(a, b, ss.at[h, j, k, n], rs.at[(h,) + at], f, to)

    def start_copies():
        result = []
        for h in range(2):
            first = (ys, zs)[h]
            slot = slot_of(h, 0, 0)
            result.append(kv_copy(h, 0, 0, 0, own.at[h], slot, (1, 0, 0), first(1)))
            result.append(kv_copy(h, 0, 0, 1, own.at[h], slot, (3, 0, 0), first(3)))
        return result

    def pass_copies(j):
        result = []
        for h in range(2):
            second = (zs, ys)[h]
            slot = slot_of(h, j, 0)
            full = own.at[h] if j == 0 else slot
            result.append(kv_copy(h, j, 0, 2, full, slot, (j, 1, 0), second(1)))
            result.append(kv_copy(h, j, 0, 3, full, slot, (j, 3, 0), second(3)))
        return result

    def relay_copies(j, k):
        result = []
        for h in range(2):
            first, second = (ys, zs) if h == 0 else (zs, ys)
            n, at, to = (j // 2, (2, 0), first(j)) if k == 0 else (k // 2, (j, 2), second(k))
            part = half_of(slot_of(h, j, k), n)
            result.append(kv_copy(h, j, k, 0, part, part, at + (n,), to))
        return result

    def copies_at(n):
        j, k = ORDER[n]
        relayed = RELAYED.get(n, ((j, k),) if k in (1, 3) else ())
        result = []
        for jj, kk in relayed:
            result += relay_copies(jj, kk)
        for jj in PASSED.get(n, ()):
            result += pass_copies(jj)
        return result

    def landed(dst, recv):
        remote(dst, dst, local.at[0], recv, fp, s).wait_recv()

    def take(j, k):
        for h in range(2):
            slot = slot_of(h, j, k)
            if k == 2 or (j == 2 and k == 0):
                landed(half_of(slot, 0), rs.at[h, j, k, 0])
                landed(half_of(slot, 1), rs.at[h, j, k, 1])
            else:
                landed(slot, rs.at[h, j, k, 0])

    for copy in brought:
        copy.wait()
    for copy in start_copies():
        copy.start()
    lower, upper = pl.ds(0, 128), pl.ds(128, 128)
    parts = [
        remote(wo_half.at[0], wog.at[2, lower], oss.at[0], ors.at[0], xs(1), s),
        remote(wo_half.at[1], wog.at[2, upper], oss.at[1], ors.at[1], xs(3), s),
        remote(wo.at[upper], wog.at[3, upper], oss.at[2], ors.at[2], xs(1), s),
        remote(wo.at[lower], wog.at[1, lower], oss.at[3], ors.at[3], xs(3), s),
    ]
    keeps = [
        pltpu.make_async_copy(wo, wog.at[0], local.at[1]),
        pltpu.make_async_copy(wo_half.at[0], wog.at[3, lower], local.at[2]),
        pltpu.make_async_copy(wo_half.at[1], wog.at[1, upper], local.at[3]),
    ]
    for copy in parts + keeps:
        copy.start()
    kv[0, s] = own[0]
    kv[1, s] = own[1]
    top[...] = jnp.full_like(top, NEG)
    den[...] = jnp.zeros_like(den)
    acc[...] = jnp.zeros_like(acc)

    def step(i, carry):
        j = k = 0
        for n, (jj, kk) in enumerate(ORDER):
            if n > 0:
                j = jnp.where(i == n, jj, j)
                k = jnp.where(i == n, kk, k)

                @pl.when(i == n)
                def _(n=n, jj=jj, kk=kk):
                    for at in TAKEN.get(n, ((jj, kk),)):
                        take(*at)
                    for copy in copies_at(n):
                        copy.start()

        a = (y + 4 - j) % 4 * 4 + (z + 4 - k) % 4
        b = (y + 4 - k) % 4 * 4 + (z + 4 - j) % 4
        at = functools.partial(attend, q, acc, top, den)
        inc = jnp.where(a <= s, 1, 0)
        at(kv.at[0, a], 0, 256, 0, inc)
        at(kv.at[0, a], 1, 512, 256, inc)
        at(kv.at[0, a], 2, 512, None, inc)
        at(kv.at[0, a], 3, 512, None, inc)
        inc = jnp.where(b <= s, 1, 0)
        at(kv.at[1, b], 2, 256, 0, inc)
        at(kv.at[1, b], 3, 512, 256, inc)
        return carry

    lax.fori_loop(0, 16, step, 0)
    for tile in range(4):
        block = (acc[tile] / den[tile]).astype(BF)
        for head in range(2):
            for owner in range(8):
                start = head * 256 + owner * 32
                ctx[owner // 2, owner % 2, tile, head] = block[start : start + 32]
    for copy in start_copies():
        copy.wait_send()
    for n in range(1, 16):
        for copy in copies_at(n):
            copy.wait_send()
    x = f // 2
    far = (x + 2) % 4
    last = [
        remote(ctx.at[far, 0], via.at[0], css.at[0], crs.at[0], xs(1), s),
        remote(ctx.at[far, 1], via.at[1], css.at[1], crs.at[1], xs(3), s),
        remote(ctx.at[(x + 1) % 4], seen.at[3], css.at[2], crs.at[2], xs(1), s),
        remote(ctx.at[(x + 3) % 4], seen.at[1], css.at[3], crs.at[3], xs(3), s),
        remote(via.at[0], seen.at[2, 0], css.at[4], crs.at[4], xs(1), s),
        remote(via.at[1], seen.at[2, 1], css.at[5], crs.at[5], xs(3), s),
    ]
    for copy in last[:4]:
        copy.start()
    seen[0] = ctx[x]
    for n in range(2):
        landed(via.at[n], crs.at[n])
        last[4 + n].start()
    for copy in keeps:
        copy.wait()
    for copy in parts:
        copy.wait()
    landed(seen.at[3], crs.at[2])
    landed(seen.at[1], crs.at[3])
    landed(seen.at[2, 0], crs.at[4])
    landed(seen.at[2, 1], crs.at[5])
    for d in range(4):
        for head in range(2):
            cols = slice(d * 256 + head * 128, d * 256 + head * 128 + 128)
            for owner in range(2):
                lhs[owner, :, cols] = seen[d, owner, :, head].reshape(128, 128)

    def columns(c):
        return pl.ds(pl.multiple_of(c * 512, 128), 512)

    def share(c):
        return remote(
            give.at[:, columns(c)], got.at[:, columns(c)], gss.at[c], grs.at[c], fp, s
        )

    def partial(owner, c):
        return jnp.dot(
            lhs[owner], wog[:, :, columns(c)].reshape(1024, 512), preferred_element_type=F32
        )

    def to_partner(c, carry):
        give[:, columns(c)] = partial(1 - core, c).astype(BF)

        @pl.when(c > 0)
        def _():
            share(c - 1).start()

        return carry

    def to_output(c, carry):
        mine = partial(core, c)

        @pl.when(c == 0)
        def _():
            share(7).start()

        share(c).wait()
        out[:, columns(c)] = (mine + got[:, columns(c)].astype(F32)).astype(BF)
        return carry

    lax.fori_loop(0, 8, to_partner, 0)
    lax.fori_loop(0, 8, to_output, 0)
    for copy in last:
        copy.wait_send()


def attention(q, own, wo, wo_half):
    dma = pltpu.SemaphoreType.DMA
    vmem = pl.BlockSpec(memory_space=pltpu.VMEM)
    hbm = pl.BlockSpec(memory_space=pl.ANY)
    state = pltpu.VMEM((4, 512, 128), F32)
    return pl.pallas_call(
        attention_kernel,
        out_shape=jax.ShapeDtypeStruct((128, 4096), BF),
        in_specs=[hbm] * 4,
        out_specs=vmem,
        scratch_shapes=[
            pltpu.VMEM((4, 512, 128), BF),
            pltpu.VMEM((2, 512, 256), BF),
            pltpu.VMEM((2, 16, 512, 256), BF),
            state,
            state,
            state,
            pltpu.VMEM((4, 2, 4, 2, 32, 128), BF),
            pltpu.VMEM((4, 2, 4, 2, 32, 128), BF),
            pltpu.VMEM((2, 4, 2, 32, 128), BF),
            pltpu.VMEM((2, 128, 1024), BF),
            pltpu.VMEM((4, 256, 4096), BF),
            pltpu.VMEM((128, 4096), BF),
            pltpu.VMEM((128, 4096), BF),
            dma((6,)),
            dma((2, 4, 4, 4)),
            dma((2, 4, 4, 2)),
            dma((6,)),
            dma((6,)),
            dma((4,)),
            dma((4,)),
            dma((8,)),
            dma((8,)),
        ],
        compiler_params=pltpu.CompilerParams(
            collective_id=3, has_side_effects=True, vmem_limit_bytes=63 << 20
        ),
        name="attention",
    )(q, own, wo, wo_half)


def per_device(
    vit_states,
    frame_slot,
    patch_count,
    vis_start,
    text_embed,
    vit_ln_gain,
    vit_ln_bias,
    vit_qkv_w,
    vit_qkv_b,
    vit_out_w,
    vit_out_b,
    proj_w,
    proj_b,
    attn_gain,
    wq,
    wk,
    wv,
    wo,
):
    s = lax.axis_index("seq")
    exponents = jnp.arange(0, 128, 2).astype(F32) / 128
    inverse = jnp.power(F32(ROPE_THETA), -exponents)
    steps = jnp.concatenate([jnp.arange(128) * 128, jnp.arange(8) * 16 + s]).astype(F32)
    angles = steps[:, None] * jnp.concatenate([inverse, inverse])[None, :]
    trig = jnp.stack([jnp.cos(angles), jnp.sin(angles)])
    queries, own, wo_half = front(
        [frame_slot[None], patch_count[None], vis_start[None]],
        [
            vit_states,
            vit_qkv_w,
            vit_out_w,
            text_embed.reshape(128, 4096),
            vit_ln_gain,
            vit_ln_bias,
            vit_out_b,
            vit_qkv_b,
            proj_b,
            attn_gain,
            trig,
        ],
        [proj_w, wq, wk, wv, wo],
    )
    return attention(queries, own, wo, wo_half).reshape(128, 1, 4096)


def solution(mesh):
    return jax.shard_map(
        per_device,
        mesh=mesh,
        in_specs=(
            P(("frame", "seq"), None, None),
            P(),
            P(),
            P(),
            P(None, ("frame", "seq"), None),
            P(),
            P(),
            P("seq", None),
            P(),
            P("seq", None),
            P(),
            P(),
            P(),
            P(),
            P(None, "frame"),
            P(None, "frame"),
            P(None, "frame"),
            P("frame", None),
        ),
        out_specs=P(None, ("frame", "seq"), None),
        check_vma=False,
    )
```
